32 devices in a mesh: coil: 4 (over x, core), slab: 8 (over z, y).
Axes of the slice: x: 2, y: 2, z: 4, core: 2. Of those that a mesh axis runs over, the one named last changes fastest.
Arguments:
- kspace_data: bfloat16 [32, 2, 128, 128, 128], P('coil', None, None, 'slab'), may hold values from -4 to 4
- coil_maps: bfloat16 [32, 2, 128, 128, 128], P('coil', None, 'slab'), may hold values from -1.796875 to 1.796875
- sample_mask: int32 [32, 128, 128], P('coil', None, 'slab'), may hold values 0 or 1
- initial_image: float32 [2, 128, 128, 128], P(None, 'slab', 'coil'), may hold values from -6 to 6
Outputs:
- image: float32 [2, 128, 128, 128], P(None, 'slab', 'coil')
The draws below stay inside these ranges and needn't reach their ends.
All inputs are finite; a program needn't handle non-finite values. No bound on the sum of `sample_mask` on one device may be relied on, other than what follows from the above.
Results may differ from the reference program's by a relative error of at most 0.0045.
Values may be sent and summed in bfloat16 or wider, within the bound.
A program may use at most 128 MiB of HBM per device.

```python
import math
import jax
import jax.numpy as jnp
from jax import lax

NX = 128
NY = 128
NZ = 128
COILS = 32
ITERS = 2


def touch_ends(entries, own_key, smallest, top_value):
    dims = entries.shape
    spot = [jax.random.randint(jax.random.fold_in(own_key, axis), (), 0, dims[axis]) for axis in range(len(dims))]
    entries = entries.at[tuple(spot)].set(smallest)
    longest = dims.index(max(dims))
    spot[longest] = (spot[longest] + 1) % dims[longest]
    return entries.at[tuple(spot)].set(top_value)


def spiked(entries, rng, source, target, blocks, factor):
    owner, partner = [(jnp.arange(entries.shape[axis_at]) // (entries.shape[axis_at] // blocks)).reshape([-1 if axis == axis_at else 1 for axis in range(entries.ndim)]) for axis_at in (source, target)]
    chosen = jax.random.permutation(rng, blocks)[partner]
    strong = (owner == chosen) | (owner == (partner + blocks // 2) % blocks)
    return jnp.where(strong, factor * entries, entries)


def block_scale(stream_key, dims, cuts, low, high):
    loudness = 1.0
    for position, shards_of in cuts:
        heights = jax.random.uniform(jax.random.fold_in(jax.random.fold_in(stream_key, 6), position), (shards_of,), jnp.float32, low / len(cuts), high / len(cuts))
        loudness = loudness * jnp.repeat(jnp.exp(heights), dims[position] // shards_of).reshape((-1,) + (1,) * (len(dims) - 1 - position))
    return loudness


def normal_values(stream_key, shape, scale, limit, cuts=(), kind=jnp.bfloat16):
    level = block_scale(stream_key, shape, cuts, -0.22, 0.18) if cuts else 1.0
    entries = jax.random.normal(stream_key, shape, jnp.float32) * scale * level
    return jnp.minimum(jnp.maximum(entries, -limit), limit).astype(kind)


def bell_draw_with(rng, shape, scale, bound, cuts, heavy, kind=jnp.bfloat16):
    array = scale * jax.random.normal(rng, shape, jnp.float32)
    if cuts:
        array = array * block_scale(rng, shape, cuts, -0.22, 0.18)
    return jnp.clip(spiked(array, jax.random.fold_in(rng, 3), *heavy), -bound, bound).astype(kind)


def setup_inputs(seed: int = 0) -> dict:
    key_list = jax.random.split(jax.random.key(seed), 5)
    kspace_data = normal_values(key_list[0], (COILS, 2, NZ, NY, NX), 0.5, 4.0, ((0, 4), (3, 8)))
    coil_maps = bell_draw_with(key_list[1], (COILS, 2, NZ, NY, NX), 0.3, 1.796875, ((0, 4), (2, 8)), (0, 3, 4, 2.0))
    sample_mask = touch_ends((jax.random.randint(key_list[2], (COILS, NZ, NY), 0, 3) < 1).astype(jnp.int32), jax.random.fold_in(key_list[2], 1), 0, 1)
    initial_image = normal_values(key_list[3], (2, NZ, NY, NX), 1.0, 6.0, ((1, 8), (2, 4)), jnp.float32)
    return {"kspace_data": kspace_data, "coil_maps": coil_maps, "sample_mask": sample_mask, "initial_image": initial_image}


dual_step = 0.25
primal_step = 0.25
tv_weight = 0.5

def dft_table(length, inverse):
    counter = jnp.arange(length, dtype=jnp.int32)
    product = counter[:, None] * counter[None, :] % length
    phase = 2.0 * math.pi / length * product.astype(jnp.float32)
    scale = 1.0 / math.sqrt(length)
    real_part = jnp.cos(phase) * scale
    imag_part = jnp.sin(phase) * scale
    if not inverse:
        imag_part = -imag_part
    table = jnp.stack([jnp.stack([real_part, imag_part]), jnp.stack([-imag_part, real_part])])
    return table.astype(jnp.bfloat16)

def along_x(field, table):
    return jnp.einsum('kzyx,kjxw->jzyw', field.astype(jnp.float32), table.astype(jnp.float32))

def along_y(field, table):
    return jnp.einsum('kzyx,kjyv->jzvx', field.astype(jnp.float32), table.astype(jnp.float32))

def along_z(field, table):
    return jnp.einsum('kzyx,kjzw->jwyx', field.astype(jnp.float32), table.astype(jnp.float32))

def forward_diff(field, axis_pos):
    length = field.shape[axis_pos]
    upper = lax.slice_in_dim(field, 1, length, axis=axis_pos)
    lower = lax.slice_in_dim(field, 0, length - 1, axis=axis_pos)
    zero_slice = jnp.zeros_like(lax.slice_in_dim(field, 0, 1, axis=axis_pos))
    return jnp.concatenate([upper - lower, zero_slice], axis_pos)

def backward_diff(field, axis_pos):
    length = field.shape[axis_pos]
    lower = lax.slice_in_dim(field, 0, length - 1, axis=axis_pos)
    zero_slice = jnp.zeros_like(lax.slice_in_dim(field, 0, 1, axis=axis_pos))
    return jnp.concatenate([zero_slice, lower], axis_pos) - field

def reference(kspace_data, coil_maps, sample_mask, initial_image):
    forward_x = dft_table(NX, False)
    forward_y = dft_table(NY, False)
    forward_z = dft_table(NZ, False)
    inverse_x = dft_table(NX, True)
    inverse_y = dft_table(NY, True)
    inverse_z = dft_table(NZ, True)
    current = initial_image
    guess = initial_image
    dual_data = jnp.zeros(kspace_data.shape, jnp.float32)
    duals = (jnp.zeros_like(current), jnp.zeros_like(current), jnp.zeros_like(current))
    for turn_index in range(ITERS):

        def per_coil(total, items):
            maps_one, data_one, mask_one, dual_one = items
            maps_real = maps_one[0].astype(jnp.float32)
            maps_imag = maps_one[1].astype(jnp.float32)
            pieces = jnp.stack([maps_real * guess[0] - maps_imag * guess[1], maps_real * guess[1] + maps_imag * guess[0]]).astype(jnp.bfloat16)
            pieces = along_x(pieces, forward_x).astype(jnp.bfloat16)
            pieces = along_y(pieces, forward_y).astype(jnp.bfloat16)
            spectrum = along_z(pieces, forward_z)
            sampled = mask_one[None, :, :, None].astype(jnp.float32)
            dual_new = (dual_one + dual_step * (sampled * (spectrum - data_one.astype(jnp.float32)))) / (1.0 + dual_step)
            back_field = along_z(dual_new.astype(jnp.bfloat16), inverse_z).astype(jnp.bfloat16)
            back_field = along_y(back_field, inverse_y).astype(jnp.bfloat16)
            back_field = along_x(back_field, inverse_x)
            combined = jnp.stack([maps_real * back_field[0] + maps_imag * back_field[1], maps_real * back_field[1] - maps_imag * back_field[0]])
            return (total + combined, dual_new)
        data_grad, dual_data = lax.scan(per_coil, jnp.zeros_like(current), (coil_maps, kspace_data, sample_mask, dual_data))
        grads = (forward_diff(guess, 1), forward_diff(guess, 2), forward_diff(guess, 3))
        moved = [duals[num] + dual_step * grads[num] for num in range(3)]
        magnitude = jnp.sqrt(lax.optimization_barrier(jnp.sum(moved[0] * moved[0], 0)) + lax.optimization_barrier(jnp.sum(moved[1] * moved[1], 0)) + lax.optimization_barrier(jnp.sum(moved[2] * moved[2], 0)))
        factor = 1.0 / jnp.maximum(1.0, magnitude / tv_weight)
        duals = (moved[0] * factor, moved[1] * factor, moved[2] * factor)
        spread = backward_diff(duals[0], 1) + backward_diff(duals[1], 2) + backward_diff(duals[2], 3)
        updated = current - primal_step * (data_grad + spread)
        guess = 2.0 * updated - current
        current = updated
    return current
```

```python
import functools
import math

import jax
import jax.numpy as jnp
import ml_dtypes
import numpy as np
from jax import lax
from jax.experimental import pallas as pl
from jax.experimental.layout import Layout, with_layout_constraint
from jax.experimental.pallas import tpu as pltpu
from jax.sharding import PartitionSpec as P

ITERS = 2

dual_step = 0.25
primal_step = 0.25
tv_weight = 0.5
f32 = jnp.float32
bf16 = jnp.bfloat16


def from_behind(block, axis, distance):
    devices = range(lax.axis_size(axis))
    route = [(i - distance, i) for i in devices if i - distance in devices]
    return lax.ppermute(block, axis, route)


def dft_table(length, inverse):
    counter = np.arange(length)
    phase = 2.0 * math.pi / length * (np.outer(counter, counter) % length)
    real_part = np.cos(phase) / math.sqrt(length)
    imag_part = np.sin(phase) / math.sqrt(length)
    if not inverse:
        imag_part = -imag_part
    table = np.stack([np.stack([real_part, imag_part]), np.stack([-imag_part, real_part])])
    return table.astype(ml_dtypes.bfloat16)


def on_right(table):
    n = table.shape[2]
    return jnp.asarray(table.transpose(0, 2, 1, 3).reshape(2 * n, 2 * n))


def on_left(table):
    n = table.shape[2]
    return jnp.asarray(table.transpose(1, 3, 0, 2).reshape(2 * n, 2 * n))


def plane(ref, coil, part):
    block = ref[:, coil, 0, part]
    return block.reshape(block.shape[0] * block.shape[1], block.shape[2])


def dot(a, b, dims=((1,), (0,))):
    return lax.dot_general(a, b, (dims, ((), ())), preferred_element_type=f32)


def combine(out_ref, maps_ref, images, group):
    nz, ny = out_ref.shape[2:]
    real_sum = imag_sum = None
    for coil in range(group):
        real = images[coil * nz : (coil + 1) * nz, :ny]
        imag = images[coil * nz : (coil + 1) * nz, ny:]
        maps_real = plane(maps_ref, coil, 0).astype(f32)
        maps_imag = plane(maps_ref, coil, 1).astype(f32)
        real_term = maps_real * real + maps_imag * imag
        imag_term = maps_real * imag - maps_imag * real
        real_sum = real_term if coil == 0 else real_sum + real_term
        imag_sum = imag_term if coil == 0 else imag_sum + imag_term

    @pl.when(pl.program_id(1) == 0)
    def _():
        out_ref[0, 0] = real_sum
        out_ref[0, 1] = imag_sum

    @pl.when(pl.program_id(1) > 0)
    def _():
        out_ref[0, 0] += real_sum
        out_ref[0, 1] += imag_sum


def normal_kernel(group, guess_ref, maps_ref, mask_ref, fy_ref, fz_ref, gz_ref, gy_ref, out_ref):
    nz, ny = out_ref.shape[2:]
    guess_real = guess_ref[0, 0]
    guess_imag = guess_ref[0, 1]
    rows = []
    for coil in range(group):
        maps_real = plane(maps_ref, coil, 0).astype(f32)
        maps_imag = plane(maps_ref, coil, 1).astype(f32)
        real = maps_real * guess_real - maps_imag * guess_imag
        imag = maps_real * guess_imag + maps_imag * guess_real
        rows.append(jnp.concatenate([real.astype(bf16), imag.astype(bf16)], 1))
    pieces = dot(jnp.concatenate(rows, 0), fy_ref[...]).astype(bf16)
    pieces = jnp.concatenate(
        [
            jnp.concatenate(
                [pieces[c * nz : (c + 1) * nz, j * ny : (j + 1) * ny] for c in range(group)], 1
            )
            for j in range(2)
        ],
        0,
    )
    spectrum = dot(fz_ref[...], pieces).astype(bf16)
    mask = jnp.concatenate([mask_ref[c] for c in range(group)], 1)
    spectrum = spectrum * jnp.concatenate([mask, mask], 0)
    pieces = dot(gz_ref[...], spectrum).astype(bf16)
    pieces = jnp.concatenate(
        [
            jnp.concatenate(
                [pieces[j * nz : (j + 1) * nz, c * ny : (c + 1) * ny] for j in range(2)], 1
            )
            for c in range(group)
        ],
        0,
    )
    combine(out_ref, maps_ref, dot(pieces, gy_ref[...]), group)


def data_kernel(group, data_ref, maps_ref, gy_ref, out_ref):
    columns = jnp.concatenate(
        [
            jnp.concatenate([plane(data_ref, c, 0), plane(data_ref, c, 1)], 0)
            for c in range(group)
        ],
        1,
    )
    combine(out_ref, maps_ref, dot(columns, gy_ref[...], ((0,), (0,))), group)


def whole(shape):
    return pl.BlockSpec(shape, lambda x, c: (0,) * len(shape))


def coil_blocks(array, group):
    src, _, _, parts, planes, cols = array.shape
    return pl.BlockSpec((src, group, 1, parts, planes, cols), lambda x, c: (0, c, x, 0, 0, 0))


def call(kernel, group, operands, specs, shape, coils, flops, nbytes):
    return pl.pallas_call(
        functools.partial(kernel, group),
        out_shape=jax.ShapeDtypeStruct(shape, f32),
        grid=(shape[0], coils // group),
        in_specs=specs,
        out_specs=pl.BlockSpec((1,) + shape[1:], lambda x, c: (x, 0, 0, 0)),
        compiler_params=pltpu.CompilerParams(
            dimension_semantics=("arbitrary", "arbitrary"), vmem_limit_bytes=48 * 2**20
        ),
        cost_estimate=pl.CostEstimate(flops=flops, bytes_accessed=nbytes, transcendentals=0),
    )(*operands)


def coil_group(coils):
    return max(g for g in (1, 2, 4) if coils % g == 0)


def apply_normal(guess, maps, mask, tables):
    coils = maps.shape[1]
    group = coil_group(coils)
    shape = guess.shape
    specs = [
        pl.BlockSpec((1,) + shape[1:], lambda x, c: (x, 0, 0, 0)),
        coil_blocks(maps, group),
        pl.BlockSpec((group,) + mask.shape[1:], lambda x, c: (c, 0, 0)),
    ] + [whole(t.shape) for t in tables]
    cells = coils * shape[0] * shape[2] * shape[3]
    return call(
        normal_kernel, group, (guess, maps, mask) + tables, specs, shape, coils, cells * 4096, cells * 4
    )


def apply_data(data, maps, table, shape):
    coils = maps.shape[1]
    group = coil_group(coils)
    specs = [coil_blocks(data, group), coil_blocks(maps, group), whole(table.shape)]
    cells = coils * shape[0] * shape[2] * shape[3]
    return call(data_kernel, group, (data, maps, table), specs, shape, coils, cells * 1024, cells * 8)


def exchange(blocks):
    got = lax.all_to_all(blocks, "slab", split_axis=0, concat_axis=0, tiled=True)
    if got.shape[4] % 16:
        src, coils, width, parts, share, cols = got.shape
        got = got.transpose(1, 2, 3, 0, 4, 5).reshape(1, coils, width, parts, src * share, cols)
    return got


def tv_update(guess, duals):
    width = guess.shape[0]
    size = lax.axis_size("slab") * width
    pos = lax.axis_index("slab") * width + lax.broadcasted_iota(jnp.int32, (width, 1, 1, 1), 0)
    ahead_x = jnp.concatenate([guess[1:], from_behind(guess[:1], "slab", -1)], 0)
    grad_x = jnp.where(pos < size - 1, ahead_x - guess, 0.0)
    grad_z = jnp.concatenate(
        [guess[:, :, 1:] - guess[:, :, :-1], jnp.zeros_like(guess[:, :, :1])], 2
    )
    grad_y = jnp.concatenate([guess[..., 1:] - guess[..., :-1], jnp.zeros_like(guess[..., :1])], 3)
    moved = [dual_step * grad for grad in (grad_z, grad_y, grad_x)]
    if duals is not None:
        moved = [dual + step for dual, step in zip(duals, moved)]
    magnitude = jnp.sqrt(sum(jnp.sum(w * w, 1, keepdims=True) for w in moved))
    factor = 1.0 / jnp.maximum(1.0, magnitude / tv_weight)
    dual_z, dual_y, dual_x = [w * factor for w in moved]
    prior = from_behind(dual_x[-1:], "slab", 1)
    spread_x = jnp.concatenate([prior, dual_x[:-1]], 0) - dual_x
    spread_z = jnp.concatenate([jnp.zeros_like(dual_z[:, :, :1]), dual_z[:, :, :-1]], 2) - dual_z
    spread_y = jnp.concatenate([jnp.zeros_like(dual_y[..., :1]), dual_y[..., :-1]], 3) - dual_y
    return (dual_z, dual_y, dual_x), spread_z + spread_y + spread_x


def on_device(kspace_data, coil_maps, sample_mask, initial_image):
    slabs = lax.axis_size("slab")
    groups = lax.axis_size("coil")
    coils, _, planes, ny, nx = coil_maps.shape
    nz = kspace_data.shape[2]
    shares = kspace_data.shape[3]
    rows = initial_image.shape[2]
    width = nx // slabs
    forward_y, inverse_y = dft_table(ny, False), dft_table(ny, True)
    forward_z, inverse_z = dft_table(nz, False), dft_table(nz, True)
    inverse_x = jnp.asarray(dft_table(nx, True))
    tables = (on_right(forward_y), on_left(forward_z), on_left(inverse_z), on_right(inverse_y))

    image = initial_image.reshape(2, planes, rows, slabs, width).transpose(3, 4, 0, 2, 1)
    image = lax.all_to_all(
        image.reshape(slabs, -1), "slab", split_axis=0, concat_axis=0, tiled=True
    ).reshape(slabs, width, 2, rows, planes)
    image = image.transpose(1, 2, 3, 0, 4).reshape(width, 2, rows, nz)
    image = lax.all_gather(image, "coil", axis=2, tiled=True).swapaxes(2, 3)
    mask = lax.all_gather(sample_mask.astype(bf16), "slab", axis=2, tiled=True)

    maps = coil_maps.reshape(coils, 2, planes, ny, slabs, width).transpose(4, 0, 5, 1, 2, 3)
    maps, image, mask = lax.optimization_barrier((maps, image, mask))
    maps = exchange(maps)

    data = kspace_data * sample_mask[:, None, :, :, None].astype(bf16)
    data = jnp.einsum("ckzyx,kjxw->cjzyw", data, inverse_x, preferred_element_type=f32).astype(bf16)
    data = jnp.einsum(
        "ckzyx,kjzw->cjywx", data, jnp.asarray(inverse_z), preferred_element_type=f32
    ).astype(bf16)
    data = data.reshape(coils, 2, shares, nz, slabs, width).transpose(4, 0, 5, 1, 2, 3)
    data, maps = lax.optimization_barrier((data, maps))
    data = exchange(data)

    normal = apply_normal(image, maps, mask, tables)
    duals, spread = tv_update(image, None)
    data, normal, duals, spread = lax.optimization_barrier((data, normal, duals, spread))
    back_data = apply_data(data, maps, tables[3], image.shape)
    scale = dual_step / (1.0 + dual_step)
    data_grad = lax.psum(scale * (normal - back_data), "coil")
    updated = image - primal_step * (data_grad + spread)
    guess = 2.0 * updated - image
    normal = apply_normal(guess, maps, mask, tables)
    _, spread = tv_update(guess, duals)
    known = updated - primal_step * (data_grad / (1.0 + dual_step) + spread)
    share = known / groups - (primal_step * scale) * (normal - back_data)
    share = lax.psum_scatter(share.swapaxes(2, 3), "coil", scatter_dimension=2, tiled=True)
    share = share.reshape(width, 2, rows, slabs, planes).transpose(3, 1, 4, 2, 0)
    share = lax.all_to_all(
        share.reshape(slabs, -1), "slab", split_axis=0, concat_axis=0, tiled=True
    ).reshape(slabs, 2, planes, rows, width)
    return share.transpose(1, 2, 3, 0, 4).reshape(2, planes, rows, nx)


def all_planes(ref, coil, part):
    block = ref[:, coil, 0, 0, part]
    return block.reshape(block.shape[0] * block.shape[1], block.shape[2])


def combine_planes(out_ref, maps, images):
    nz, ny = out_ref.shape[2:]
    real_sum = imag_sum = None
    for coil, (maps_real, maps_imag) in enumerate(maps):
        real = images[coil * nz : (coil + 1) * nz, :ny]
        imag = images[coil * nz : (coil + 1) * nz, ny:]
        real_term = maps_real * real + maps_imag * imag
        imag_term = maps_real * imag - maps_imag * real
        real_sum = real_term if coil == 0 else real_sum + real_term
        imag_sum = imag_term if coil == 0 else imag_sum + imag_term

    @pl.when(pl.program_id(1) == 0)
    def _():
        out_ref[0, 0] = real_sum
        out_ref[0, 1] = imag_sum

    @pl.when(pl.program_id(1) > 0)
    def _():
        out_ref[0, 0] += real_sum
        out_ref[0, 1] += imag_sum


def planes_of(maps_ref):
    return [
        (all_planes(maps_ref, c, 0).astype(f32), all_planes(maps_ref, c, 1).astype(f32))
        for c in range(maps_ref.shape[1])
    ]


def normal_planes(guess_ref, maps_ref, mask_ref, fy_ref, fz_ref, gz_ref, gy_ref, out_ref):
    nz, ny = out_ref.shape[2:]
    group = maps_ref.shape[1]
    guess_real = guess_ref[0, 0]
    guess_imag = guess_ref[0, 1]
    maps = planes_of(maps_ref)
    rows = []
    for maps_real, maps_imag in maps:
        real = maps_real * guess_real - maps_imag * guess_imag
        imag = maps_real * guess_imag + maps_imag * guess_real
        rows.append(jnp.concatenate([real.astype(bf16), imag.astype(bf16)], 1))
    pieces = dot(jnp.concatenate(rows, 0), fy_ref[...]).astype(bf16)
    pieces = jnp.concatenate(
        [
            jnp.concatenate(
                [pieces[c * nz : (c + 1) * nz, j * ny : (j + 1) * ny] for c in range(group)], 1
            )
            for j in range(2)
        ],
        0,
    )
    spectrum = dot(fz_ref[...], pieces).astype(bf16)
    mask = jnp.concatenate([mask_ref[c, 0] for c in range(group)], 1)
    spectrum = spectrum * jnp.concatenate([mask, mask], 0)
    pieces = dot(gz_ref[...], spectrum).astype(bf16)
    pieces = jnp.concatenate(
        [
            jnp.concatenate(
                [pieces[j * nz : (j + 1) * nz, c * ny : (c + 1) * ny] for j in range(2)], 1
            )
            for c in range(group)
        ],
        0,
    )
    combine_planes(out_ref, maps, dot(pieces, gy_ref[...]))


def data_planes(data_ref, maps_ref, gy_ref, out_ref):
    columns = jnp.concatenate(
        [
            jnp.concatenate([all_planes(data_ref, c, 0), all_planes(data_ref, c, 1)], 0)
            for c in range(data_ref.shape[1])
        ],
        1,
    )
    combine_planes(out_ref, planes_of(maps_ref), dot(columns, gy_ref[...], ((0,), (0,))))


def plane_call(kernel, operands, specs, shape, steps, flops, nbytes):
    return pl.pallas_call(
        kernel,
        out_shape=jax.ShapeDtypeStruct(shape, f32),
        grid=(shape[0], steps),
        in_specs=specs,
        out_specs=pl.BlockSpec((1,) + shape[1:], lambda x, c: (x, 0, 0, 0)),
        compiler_params=pltpu.CompilerParams(
            dimension_semantics=("arbitrary", "arbitrary"), vmem_limit_bytes=48 * 2**20
        ),
        cost_estimate=pl.CostEstimate(flops=flops, bytes_accessed=nbytes, transcendentals=0),
    )(*operands)


def every_source(array, start=0):
    slabs, groups, _, _, parts, rows, cols = array.shape
    return pl.BlockSpec(
        (slabs, groups, 1, 1, parts, rows, cols), lambda x, c: (0, 0, x, start + c, 0, 0, 0)
    )


def normal_of(guess, maps, mask, first, tables):
    shape = guess.shape
    coils = maps.shape[3]
    groups = maps.shape[1]
    specs = [
        pl.BlockSpec((1,) + shape[1:], lambda x, c: (x, 0, 0, 0)),
        every_source(maps),
        pl.BlockSpec((groups, 1) + mask.shape[2:], lambda x, c: (0, first + c, 0, 0)),
    ] + [whole(t.shape) for t in tables]
    cells = groups * coils * shape[0] * shape[2] * shape[3]
    return plane_call(
        normal_planes, (guess, maps, mask) + tables, specs, shape, coils, cells * 4096, cells * 4
    )


def back_of(data, maps, table, shape, data_start, maps_start, coils):
    specs = [every_source(data, data_start), every_source(maps, maps_start), whole(table.shape)]
    cells = maps.shape[1] * coils * shape[0] * shape[2] * shape[3]
    return plane_call(data_planes, (data, maps, table), specs, shape, coils, cells * 1024, cells * 8)


EVERY = ("slab", "coil")


def swap(blocks):
    return lax.all_to_all(blocks, EVERY, split_axis=0, concat_axis=0, tiled=True)


def tv_planes(guess, duals, first, total):
    here, ahead = guess[:-1], guess[1:]
    pos = first - 1 + lax.broadcasted_iota(jnp.int32, (here.shape[0], 1, 1, 1), 0)
    grad_x = jnp.where(pos < total - 1, ahead - here, 0.0)
    grad_z = jnp.concatenate([here[:, :, 1:] - here[:, :, :-1], jnp.zeros_like(here[:, :, :1])], 2)
    grad_y = jnp.concatenate([here[..., 1:] - here[..., :-1], jnp.zeros_like(here[..., :1])], 3)
    moved = [dual_step * grad for grad in (grad_z, grad_y, grad_x)]
    if duals is not None:
        moved = [dual + step for dual, step in zip(duals, moved)]
    magnitude = jnp.sqrt(sum(jnp.sum(w * w, 1, keepdims=True) for w in moved))
    factor = 1.0 / jnp.maximum(1.0, magnitude / tv_weight)
    duals = [w * factor for w in moved]
    dual_z, dual_y = duals[0][1:], duals[1][1:]
    dual_x = jnp.where(pos < 0, 0.0, duals[2])
    spread_x = dual_x[:-1] - dual_x[1:]
    spread_z = jnp.concatenate([jnp.zeros_like(dual_z[:, :, :1]), dual_z[:, :, :-1]], 2) - dual_z
    spread_y = jnp.concatenate([jnp.zeros_like(dual_y[..., :1]), dual_y[..., :-1]], 3) - dual_y
    return duals, spread_z + spread_y + spread_x


def by_planes(kspace_data, coil_maps, sample_mask, initial_image):
    slabs = lax.axis_size("slab")
    groups = lax.axis_size("coil")
    devices = slabs * groups
    coils, _, depth, ny, nx = coil_maps.shape
    nz, shares = kspace_data.shape[2:4]
    rows = initial_image.shape[2]
    width = nx // devices
    me = lax.axis_index(EVERY)
    forward_y, inverse_y = dft_table(ny, False), dft_table(ny, True)
    forward_z, inverse_z = dft_table(nz, False), dft_table(nz, True)
    inverse_x = jnp.asarray(dft_table(nx, True))
    tables = (on_right(forward_y), on_left(forward_z), on_left(inverse_z), on_right(inverse_y))
    few = max(1, coils // 8)
    hold = lax.optimization_barrier

    def packed(array):
        return array.reshape((devices, width) + array.shape[1:])

    def sent(array):
        return swap(array).reshape((slabs, groups) + array.shape[1:])

    def in_place(array):
        order = Layout(major_to_minor=tuple(range(array.ndim)))
        return with_layout_constraint(array, order)

    first_maps = packed(coil_maps[:few].transpose(4, 0, 1, 2, 3))
    later_maps = packed(coil_maps[few:].transpose(4, 0, 1, 2, 3))
    image = initial_image.reshape(-1, nx).astype(bf16).T.reshape(devices, width, -1)
    edge = jnp.zeros_like(image[:1, :1])
    image = jnp.concatenate(
        [
            jnp.concatenate([edge, image[:-1, -1:]], 0),
            image,
            jnp.concatenate([image[1:, :1], edge], 0),
        ],
        1,
    )
    joined = jnp.concatenate(
        [first_maps.reshape(devices, -1, ny), image.reshape(devices, -1, ny)], 1
    )
    joined = swap(joined)
    mask = lax.all_gather(sample_mask.astype(bf16), "slab", axis=2, tiled=True)
    joined, mask, later_maps = hold((joined, mask, later_maps))
    later_maps = sent(later_maps)

    image = joined[:, -image.shape[1] * image.shape[2] // ny :]
    first_maps = joined[:, : joined.shape[1] - image.shape[1]]
    first_maps = first_maps.reshape(slabs, groups, width, few, 2, depth, ny)
    image = image.reshape(slabs, groups, width + 2, 2, depth, rows)
    image = image.transpose(2, 3, 0, 4, 1, 5).reshape(width + 2, 2, nz, ny).astype(f32)
    own = image[1:-1]

    data = kspace_data * sample_mask[:, None, :, :, None].astype(bf16)
    data = jnp.einsum("ckzyx,kjxw->cjzyw", data, inverse_x, preferred_element_type=f32).astype(bf16)
    data = jnp.einsum(
        "ckzyx,kjzw->xcjyw", data, jnp.asarray(inverse_z), preferred_element_type=f32
    ).astype(bf16)
    back_edges = sorted({0, coils - few, coils})
    data = [in_place(packed(data[:, a:b])) for a, b in zip(back_edges[:-1], back_edges[1:])]
    mask, data = hold((mask, data))
    masks = []
    for half in (mask[: coils // 2], mask[coils // 2 :]):
        if masks:
            half, _ = hold((half, masks[0]))
        masks.append(lax.all_gather(half, "coil", axis=0))
    mask = jnp.concatenate(masks, 1)
    first_maps, later_maps, mask, data = hold((first_maps, later_maps, mask, data))

    maps = [(first_maps, 0), (later_maps, few)]
    scale = dual_step / (1.0 + dual_step)
    normal = sum(normal_of(own, m, mask, a, tables) for m, a in maps)
    duals, spread = tv_planes(image, None, me * width, nx)
    back = 0.0
    ready = None
    for piece, (a, b) in enumerate(zip(back_edges[:-1], back_edges[1:])):
        got = sent(data[piece])
        if ready is not None:
            back += ready
        if piece == 0:
            got, normal, duals, spread, data = hold((got, normal, duals, spread, data))
        elif piece < len(data) - 1:
            got, back, data = hold((got, back, data))
        else:
            got, back = hold((got, back))
        ready = None
        for m, start in maps:
            low, high = max(a, start), min(b, start + m.shape[3])
            if low < high:
                term = back_of(
                    got, m, tables[3], own.shape, low - a, low - start, high - low
                )
                ready = term if ready is None else ready + term
    back += ready
    data_grad = scale * (normal - back)
    change = -primal_step * (data_grad + spread)
    guess = own + 2.0 * change
    line = [g * slabs + s for s in range(slabs) for g in range(groups)]
    before = lax.ppermute(guess[-1:], ("coil", "slab"), list(zip(line[:-1], line[1:])))
    after = lax.ppermute(guess[:1], ("coil", "slab"), list(zip(line[1:], line[:-1])))
    normal = sum(normal_of(guess, m, mask, a, tables) for m, a in maps)
    _, spread = tv_planes(jnp.concatenate([before, guess, after], 0), duals, me * width, nx)
    data_grad = data_grad / (1.0 + dual_step) + scale * (normal - back)
    final = (own + change - primal_step * (data_grad + spread)).astype(bf16)
    final = final.reshape(width, 2, slabs, depth, groups, rows).transpose(2, 4, 0, 1, 3, 5)
    final = swap(final.reshape(devices, -1)).reshape(nx, -1).T
    return final.reshape(initial_image.shape).astype(f32)


def solution(mesh):
    placed = (
        P("coil", None, None, "slab", None),
        P("coil", None, "slab", None, None),
        P("coil", None, "slab"),
        P(None, "slab", "coil", None),
    )

    def on_each(kspace_data, coil_maps, sample_mask, initial_image):
        whole_planes = coil_maps.shape[4] % mesh.size == 0
        form = by_planes if whole_planes else on_device
        return form(kspace_data, coil_maps, sample_mask, initial_image)

    return jax.shard_map(
        on_each,
        mesh=mesh,
        in_specs=placed,
        out_specs=P(None, "slab", "coil", None),
        check_vma=False,
    )
```

```python
import functools
import math

import jax
import jax.numpy as jnp
import ml_dtypes
import numpy as np
from jax import lax
from jax.experimental import pallas as pl
from jax.experimental.layout import Layout, with_layout_constraint
from jax.experimental.pallas import tpu as pltpu
from jax.sharding import PartitionSpec as P

ITERS = 2

dual_step = 0.25
primal_step = 0.25
tv_weight = 0.5
f32 = jnp.float32
bf16 = jnp.bfloat16


def from_behind(block, axis, distance):
    devices = range(lax.axis_size(axis))
    route = [(i - distance, i) for i in devices if i - distance in devices]
    return lax.ppermute(block, axis, route)


def dft_table(length, inverse):
    counter = np.arange(length)
    phase = 2.0 * math.pi / length * (np.outer(counter, counter) % length)
    real_part = np.cos(phase) / math.sqrt(length)
    imag_part = np.sin(phase) / math.sqrt(length)
    if not inverse:
        imag_part = -imag_part
    table = np.stack([np.stack([real_part, imag_part]), np.stack([-imag_part, real_part])])
    return table.astype(ml_dtypes.bfloat16)


def on_right(table):
    n = table.shape[2]
    return jnp.asarray(table.transpose(0, 2, 1, 3).reshape(2 * n, 2 * n))


def on_left(table):
    n = table.shape[2]
    return jnp.asarray(table.transpose(1, 3, 0, 2).reshape(2 * n, 2 * n))


def plane(ref, coil, part):
    block = ref[:, coil, 0, part]
    return block.reshape(block.shape[0] * block.shape[1], block.shape[2])


def dot(a, b, dims=((1,), (0,))):
    return lax.dot_general(a, b, (dims, ((), ())), preferred_element_type=f32)


def combine(out_ref, maps_ref, images, group):
    nz, ny = out_ref.shape[2:]
    real_sum = imag_sum = None
    for coil in range(group):
        real = images[coil * nz : (coil + 1) * nz, :ny]
        imag = images[coil * nz : (coil + 1) * nz, ny:]
        maps_real = plane(maps_ref, coil, 0).astype(f32)
        maps_imag = plane(maps_ref, coil, 1).astype(f32)
        real_term = maps_real * real + maps_imag * imag
        imag_term = maps_real * imag - maps_imag * real
        real_sum = real_term if coil == 0 else real_sum + real_term
        imag_sum = imag_term if coil == 0 else imag_sum + imag_term

    @pl.when(pl.program_id(1) == 0)
    def _():
        out_ref[0, 0] = real_sum
        out_ref[0, 1] = imag_sum

    @pl.when(pl.program_id(1) > 0)
    def _():
        out_ref[0, 0] += real_sum
        out_ref[0, 1] += imag_sum


def normal_kernel(group, guess_ref, maps_ref, mask_ref, fy_ref, fz_ref, gz_ref, gy_ref, out_ref):
    nz, ny = out_ref.shape[2:]
    guess_real = guess_ref[0, 0]
    guess_imag = guess_ref[0, 1]
    rows = []
    for coil in range(group):
        maps_real = plane(maps_ref, coil, 0).astype(f32)
        maps_imag = plane(maps_ref, coil, 1).astype(f32)
        real = maps_real * guess_real - maps_imag * guess_imag
        imag = maps_real * guess_imag + maps_imag * guess_real
        rows.append(jnp.concatenate([real.astype(bf16), imag.astype(bf16)], 1))
    pieces = dot(jnp.concatenate(rows, 0), fy_ref[...]).astype(bf16)
    pieces = jnp.concatenate(
        [
            jnp.concatenate(
                [pieces[c * nz : (c + 1) * nz, j * ny : (j + 1) * ny] for c in range(group)], 1
            )
            for j in range(2)
        ],
        0,
    )
    spectrum = dot(fz_ref[...], pieces).astype(bf16)
    mask = jnp.concatenate([mask_ref[c] for c in range(group)], 1)
    spectrum = spectrum * jnp.concatenate([mask, mask], 0)
    pieces = dot(gz_ref[...], spectrum).astype(bf16)
    pieces = jnp.concatenate(
        [
            jnp.concatenate(
                [pieces[j * nz : (j + 1) * nz, c * ny : (c + 1) * ny] for j in range(2)], 1
            )
            for c in range(group)
        ],
        0,
    )
    combine(out_ref, maps_ref, dot(pieces, gy_ref[...]), group)


def data_kernel(group, data_ref, maps_ref, gy_ref, out_ref):
    columns = jnp.concatenate(
        [
            jnp.concatenate([plane(data_ref, c, 0), plane(data_ref, c, 1)], 0)
            for c in range(group)
        ],
        1,
    )
    combine(out_ref, maps_ref, dot(columns, gy_ref[...], ((0,), (0,))), group)


def whole(shape):
    return pl.BlockSpec(shape, lambda x, c: (0,) * len(shape))


def coil_blocks(array, group):
    src, _, _, parts, planes, cols = array.shape
    return pl.BlockSpec((src, group, 1, parts, planes, cols), lambda x, c: (0, c, x, 0, 0, 0))


def call(kernel, group, operands, specs, shape, coils, flops, nbytes):
    return pl.pallas_call(
        functools.partial(kernel, group),
        out_shape=jax.ShapeDtypeStruct(shape, f32),
        grid=(shape[0], coils // group),
        in_specs=specs,
        out_specs=pl.BlockSpec((1,) + shape[1:], lambda x, c: (x, 0, 0, 0)),
        compiler_params=pltpu.CompilerParams(
            dimension_semantics=("arbitrary", "arbitrary"), vmem_limit_bytes=48 * 2**20
        ),
        cost_estimate=pl.CostEstimate(flops=flops, bytes_accessed=nbytes, transcendentals=0),
    )(*operands)


def coil_group(coils):
    return max(g for g in (1, 2, 4) if coils % g == 0)


def apply_normal(guess, maps, mask, tables):
    coils = maps.shape[1]
    group = coil_group(coils)
    shape = guess.shape
    specs = [
        pl.BlockSpec((1,) + shape[1:], lambda x, c: (x, 0, 0, 0)),
        coil_blocks(maps, group),
        pl.BlockSpec((group,) + mask.shape[1:], lambda x, c: (c, 0, 0)),
    ] + [whole(t.shape) for t in tables]
    cells = coils * shape[0] * shape[2] * shape[3]
    return call(
        normal_kernel, group, (guess, maps, mask) + tables, specs, shape, coils, cells * 4096, cells * 4
    )


def apply_data(data, maps, table, shape):
    coils = maps.shape[1]
    group = coil_group(coils)
    specs = [coil_blocks(data, group), coil_blocks(maps, group), whole(table.shape)]
    cells = coils * shape[0] * shape[2] * shape[3]
    return call(data_kernel, group, (data, maps, table), specs, shape, coils, cells * 1024, cells * 8)


def exchange(blocks):
    got = lax.all_to_all(blocks, "slab", split_axis=0, concat_axis=0, tiled=True)
    if got.shape[4] % 16:
        src, coils, width, parts, share, cols = got.shape
        got = got.transpose(1, 2, 3, 0, 4, 5).reshape(1, coils, width, parts, src * share, cols)
    return got


def tv_update(guess, duals):
    width = guess.shape[0]
    size = lax.axis_size("slab") * width
    pos = lax.axis_index("slab") * width + lax.broadcasted_iota(jnp.int32, (width, 1, 1, 1), 0)
    ahead_x = jnp.concatenate([guess[1:], from_behind(guess[:1], "slab", -1)], 0)
    grad_x = jnp.where(pos < size - 1, ahead_x - guess, 0.0)
    grad_z = jnp.concatenate(
        [guess[:, :, 1:] - guess[:, :, :-1], jnp.zeros_like(guess[:, :, :1])], 2
    )
    grad_y = jnp.concatenate([guess[..., 1:] - guess[..., :-1], jnp.zeros_like(guess[..., :1])], 3)
    moved = [dual_step * grad for grad in (grad_z, grad_y, grad_x)]
    if duals is not None:
        moved = [dual + step for dual, step in zip(duals, moved)]
    magnitude = jnp.sqrt(sum(jnp.sum(w * w, 1, keepdims=True) for w in moved))
    factor = 1.0 / jnp.maximum(1.0, magnitude / tv_weight)
    dual_z, dual_y, dual_x = [w * factor for w in moved]
    prior = from_behind(dual_x[-1:], "slab", 1)
    spread_x = jnp.concatenate([prior, dual_x[:-1]], 0) - dual_x
    spread_z = jnp.concatenate([jnp.zeros_like(dual_z[:, :, :1]), dual_z[:, :, :-1]], 2) - dual_z
    spread_y = jnp.concatenate([jnp.zeros_like(dual_y[..., :1]), dual_y[..., :-1]], 3) - dual_y
    return (dual_z, dual_y, dual_x), spread_z + spread_y + spread_x


def on_device(kspace_data, coil_maps, sample_mask, initial_image):
    slabs = lax.axis_size("slab")
    groups = lax.axis_size("coil")
    coils, _, planes, ny, nx = coil_maps.shape
    nz = kspace_data.shape[2]
    shares = kspace_data.shape[3]
    rows = initial_image.shape[2]
    width = nx // slabs
    forward_y, inverse_y = dft_table(ny, False), dft_table(ny, True)
    forward_z, inverse_z = dft_table(nz, False), dft_table(nz, True)
    inverse_x = jnp.asarray(dft_table(nx, True))
    tables = (on_right(forward_y), on_left(forward_z), on_left(inverse_z), on_right(inverse_y))

    image = initial_image.reshape(2, planes, rows, slabs, width).transpose(3, 4, 0, 2, 1)
    image = lax.all_to_all(
        image.reshape(slabs, -1), "slab", split_axis=0, concat_axis=0, tiled=True
    ).reshape(slabs, width, 2, rows, planes)
    image = image.transpose(1, 2, 3, 0, 4).reshape(width, 2, rows, nz)
    image = lax.all_gather(image, "coil", axis=2, tiled=True).swapaxes(2, 3)
    mask = lax.all_gather(sample_mask.astype(bf16), "slab", axis=2, tiled=True)

    maps = coil_maps.reshape(coils, 2, planes, ny, slabs, width).transpose(4, 0, 5, 1, 2, 3)
    maps, image, mask = lax.optimization_barrier((maps, image, mask))
    maps = exchange(maps)

    data = kspace_data * sample_mask[:, None, :, :, None].astype(bf16)
    data = jnp.einsum("ckzyx,kjxw->cjzyw", data, inverse_x, preferred_element_type=f32).astype(bf16)
    data = jnp.einsum(
        "ckzyx,kjzw->cjywx", data, jnp.asarray(inverse_z), preferred_element_type=f32
    ).astype(bf16)
    data = data.reshape(coils, 2, shares, nz, slabs, width).transpose(4, 0, 5, 1, 2, 3)
    data, maps = lax.optimization_barrier((data, maps))
    data = exchange(data)

    normal = apply_normal(image, maps, mask, tables)
    duals, spread = tv_update(image, None)
    data, normal, duals, spread = lax.optimization_barrier((data, normal, duals, spread))
    back_data = apply_data(data, maps, tables[3], image.shape)
    scale = dual_step / (1.0 + dual_step)
    data_grad = lax.psum(scale * (normal - back_data), "coil")
    updated = image - primal_step * (data_grad + spread)
    guess = 2.0 * updated - image
    normal = apply_normal(guess, maps, mask, tables)
    _, spread = tv_update(guess, duals)
    known = updated - primal_step * (data_grad / (1.0 + dual_step) + spread)
    share = known / groups - (primal_step * scale) * (normal - back_data)
    share = lax.psum_scatter(share.swapaxes(2, 3), "coil", scatter_dimension=2, tiled=True)
    share = share.reshape(width, 2, rows, slabs, planes).transpose(3, 1, 4, 2, 0)
    share = lax.all_to_all(
        share.reshape(slabs, -1), "slab", split_axis=0, concat_axis=0, tiled=True
    ).reshape(slabs, 2, planes, rows, width)
    return share.transpose(1, 2, 3, 0, 4).reshape(2, planes, rows, nx)


def all_planes(ref, coil, part):
    block = ref[:, coil, 0, 0, part]
    return block.reshape(block.shape[0] * block.shape[1], block.shape[2])


def combine_planes(out_ref, maps, images):
    nz, ny = out_ref.shape[2:]
    real_sum = imag_sum = None
    for coil, (maps_real, maps_imag) in enumerate(maps):
        real = images[coil * nz : (coil + 1) * nz, :ny]
        imag = images[coil * nz : (coil + 1) * nz, ny:]
        real_term = maps_real * real + maps_imag * imag
        imag_term = maps_real * imag - maps_imag * real
        real_sum = real_term if coil == 0 else real_sum + real_term
        imag_sum = imag_term if coil == 0 else imag_sum + imag_term

    @pl.when(pl.program_id(1) == 0)
    def _():
        out_ref[0, 0] = real_sum
        out_ref[0, 1] = imag_sum

    @pl.when(pl.program_id(1) > 0)
    def _():
        out_ref[0, 0] += real_sum
        out_ref[0, 1] += imag_sum


def planes_of(maps_ref):
    return [
        (all_planes(maps_ref, c, 0).astype(f32), all_planes(maps_ref, c, 1).astype(f32))
        for c in range(maps_ref.shape[1])
    ]


def normal_planes(guess_ref, maps_ref, mask_ref, fy_ref, fz_ref, gz_ref, gy_ref, out_ref):
    nz, ny = out_ref.shape[2:]
    group = maps_ref.shape[1]
    guess_real = guess_ref[0, 0]
    guess_imag = guess_ref[0, 1]
    maps = planes_of(maps_ref)
    rows = []
    for maps_real, maps_imag in maps:
        real = maps_real * guess_real - maps_imag * guess_imag
        imag = maps_real * guess_imag + maps_imag * guess_real
        rows.append(jnp.concatenate([real.astype(bf16), imag.astype(bf16)], 1))
    pieces = dot(jnp.concatenate(rows, 0), fy_ref[...]).astype(bf16)
    pieces = jnp.concatenate(
        [
            jnp.concatenate(
                [pieces[c * nz : (c + 1) * nz, j * ny : (j + 1) * ny] for c in range(group)], 1
            )
            for j in range(2)
        ],
        0,
    )
    spectrum = dot(fz_ref[...], pieces).astype(bf16)
    mask = jnp.concatenate([mask_ref[c, 0] for c in range(group)], 1)
    spectrum = spectrum * jnp.concatenate([mask, mask], 0)
    pieces = dot(gz_ref[...], spectrum).astype(bf16)
    pieces = jnp.concatenate(
        [
            jnp.concatenate(
                [pieces[j * nz : (j + 1) * nz, c * ny : (c + 1) * ny] for j in range(2)], 1
            )
            for c in range(group)
        ],
        0,
    )
    combine_planes(out_ref, maps, dot(pieces, gy_ref[...]))


def back_planes(out_ref, maps_ref, gz_ref, gy_ref, spectra):
    nz, ny = out_ref.shape[2:]
    shares = spectra[0][0].shape[0]
    spectrum = jnp.concatenate([jnp.concatenate(parts, 1) for parts in spectra], 0)
    pieces = dot(spectrum, gz_ref[...]).astype(bf16)
    columns = jnp.concatenate(
        [
            jnp.concatenate(
                [
                    pieces[c * shares : (c + 1) * shares, j * nz : (j + 1) * nz]
                    for c in range(len(spectra))
                ],
                1,
            )
            for j in range(2)
        ],
        0,
    )
    combine_planes(out_ref, planes_of(maps_ref), dot(columns, gy_ref[...], ((0,), (0,))))


def dense_kernel(data_ref, maps_ref, gz_ref, gy_ref, out_ref):
    spectra = [
        (all_planes(data_ref, c, 0), all_planes(data_ref, c, 1)) for c in range(data_ref.shape[1])
    ]
    back_planes(out_ref, maps_ref, gz_ref, gy_ref, spectra)


def lanes_at(array, place):
    return jnp.take_along_axis(array, place, 1, mode="promise_in_bounds")


def sparse_kernel(data_ref, code_ref, maps_ref, gz_ref, gy_ref, out_ref):
    half = data_ref.shape[4] // 2
    spectra = []
    for coil in range(data_ref.shape[1]):
        lines = data_ref[:, coil, 0, 0].astype(f32)
        lines = [
            lines[:, j * half : (j + 1) * half].reshape(-1, lines.shape[2]) for j in range(2)
        ]
        count = lines[0].shape[0]
        codes = [code_ref[coil, 0, h * count : (h + 1) * count] for h in range(2)]
        spectra.append(
            [
                jnp.concatenate(
                    [
                        jnp.where(code >= 0, lanes_at(line, jnp.maximum(code, 0)), 0.0)
                        for code in codes
                    ],
                    0,
                ).astype(bf16)
                for line in lines
            ]
        )
    back_planes(out_ref, maps_ref, gz_ref, gy_ref, spectra)


def select_kernel(pick_ref, data_ref, out_ref):
    half = data_ref.shape[3] // 2
    lanes = data_ref.shape[4]

    def one(plane_index, _):
        for coil in range(data_ref.shape[1]):
            pick = pick_ref[coil]
            later = pick >= lanes
            place = jnp.where(later, pick - lanes, pick)
            parts = []
            for part in range(2):
                lines = data_ref[plane_index, coil, part].astype(f32)
                parts.append(
                    jnp.where(later, lanes_at(lines[half:], place), lanes_at(lines[:half], place))
                )
            out_ref[plane_index, coil] = jnp.concatenate(parts, 0).astype(bf16)
        return 0

    lax.fori_loop(0, data_ref.shape[0], one, 0)


def selected(data, pick):
    planes, coils, _, shares, lanes = data.shape
    step = max(n for n in (1, 2, 4, 8) if planes % n == 0)
    return pl.pallas_call(
        select_kernel,
        out_shape=jax.ShapeDtypeStruct((planes, coils, shares, lanes), bf16),
        grid=(planes // step,),
        in_specs=[
            pl.BlockSpec(pick.shape, lambda x: (0, 0, 0)),
            pl.BlockSpec((step,) + data.shape[1:], lambda x: (x, 0, 0, 0, 0)),
        ],
        out_specs=pl.BlockSpec((step, coils, shares, lanes), lambda x: (x, 0, 0, 0)),
        compiler_params=pltpu.CompilerParams(dimension_semantics=("arbitrary",)),
        cost_estimate=pl.CostEstimate(
            flops=data.size * 64, bytes_accessed=data.size * 3, transcendentals=0
        ),
    )(pick, data)


def share_kernel(own_ref, all_ref, send_sem, recv_sem):
    count = lax.axis_size("slab")
    slab, coil = lax.axis_index("slab"), lax.axis_index("coil")

    def device(step):
        return (coil, lax.rem(slab + step, count))

    barrier = pltpu.get_barrier_semaphore()
    for step in range(1, count):
        pl.semaphore_signal(
            barrier, inc=1, device_id=device(step), device_id_type=pl.DeviceIdType.MESH
        )
    pl.semaphore_wait(barrier, count - 1)
    copies = [
        pltpu.make_async_remote_copy(
            own_ref,
            all_ref.at[slab],
            send_sem.at[step - 1],
            recv_sem.at[step - 1],
            device_id=device(step),
            device_id_type=pl.DeviceIdType.MESH,
        )
        for step in range(1, count)
    ]
    for copy in copies:
        copy.start()
    all_ref[slab] = own_ref[...]
    for copy in copies:
        copy.wait()


def shared(own, slabs):
    return pl.pallas_call(
        share_kernel,
        out_shape=jax.ShapeDtypeStruct((slabs,) + own.shape, own.dtype),
        in_specs=[pl.BlockSpec(memory_space=pltpu.VMEM)],
        out_specs=pl.BlockSpec(memory_space=pltpu.VMEM),
        scratch_shapes=[
            pltpu.SemaphoreType.DMA((slabs - 1,)),
            pltpu.SemaphoreType.DMA((slabs - 1,)),
        ],
        compiler_params=pltpu.CompilerParams(collective_id=0, has_side_effects=True),
        cost_estimate=pl.CostEstimate(
            flops=own.size * 64, bytes_accessed=own.size * 32, transcendentals=0
        ),
    )(own)


def plane_call(kernel, operands, specs, shape, steps, flops, nbytes):
    return pl.pallas_call(
        kernel,
        out_shape=jax.ShapeDtypeStruct(shape, f32),
        grid=(shape[0], steps),
        in_specs=specs,
        out_specs=pl.BlockSpec((1,) + shape[1:], lambda x, c: (x, 0, 0, 0)),
        compiler_params=pltpu.CompilerParams(
            dimension_semantics=("arbitrary", "arbitrary"), vmem_limit_bytes=48 * 2**20
        ),
        cost_estimate=pl.CostEstimate(flops=flops, bytes_accessed=nbytes, transcendentals=0),
    )(*operands)


def every_source(array, start=0):
    slabs, groups, _, _, parts, rows, cols = array.shape
    return pl.BlockSpec(
        (slabs, groups, 1, 1, parts, rows, cols), lambda x, c: (0, 0, x, start + c, 0, 0, 0)
    )


def normal_of(guess, maps, mask, first, tables):
    shape = guess.shape
    coils = maps.shape[3]
    groups = maps.shape[1]
    specs = [
        pl.BlockSpec((1,) + shape[1:], lambda x, c: (x, 0, 0, 0)),
        every_source(maps),
        pl.BlockSpec((groups, 1) + mask.shape[2:], lambda x, c: (0, first + c, 0, 0)),
    ] + [whole(t.shape) for t in tables]
    cells = groups * coils * shape[0] * shape[2] * shape[3]
    return plane_call(
        normal_planes, (guess, maps, mask) + tables, specs, shape, coils, cells * 4096, cells * 4
    )


def back_of(data, code, maps, tables, shape, start):
    coils = data.shape[3]
    groups = maps.shape[1]
    operands, specs = [data], []
    if code is None:
        specs.append(every_source(data))
    else:
        slabs, _, _, _, shares, lanes = data.shape
        specs.append(
            pl.BlockSpec(
                (slabs, groups, 1, 1, shares, lanes), lambda x, c: (0, 0, x, c, 0, 0)
            )
        )
        operands.append(code[0])
        first = code[1]
        specs.append(
            pl.BlockSpec((groups, 1) + code[0].shape[2:], lambda x, c: (0, first + c, 0, 0))
        )
    operands += (maps,) + tables
    specs += [every_source(maps, start)] + [whole(t.shape) for t in tables]
    cells = groups * coils * shape[0] * shape[2] * shape[3]
    kernel = dense_kernel if code is None else sparse_kernel
    return plane_call(kernel, operands, specs, shape, coils, cells * 2048, cells * 8)


EVERY = ("slab", "coil")
LANES = 128
SUBLANES = 8


def ranks(flags):
    before = jnp.triu(jnp.ones((flags.shape[-1],) * 2, bf16))
    counts = jnp.einsum("...k,kl->...l", flags.astype(bf16), before, preferred_element_type=f32)
    return counts.astype(jnp.int32)


def swap(blocks):
    return lax.all_to_all(blocks, EVERY, split_axis=0, concat_axis=0, tiled=True)


def tv_planes(guess, duals, first, total):
    here, ahead = guess[:-1], guess[1:]
    pos = first - 1 + lax.broadcasted_iota(jnp.int32, (here.shape[0], 1, 1, 1), 0)
    grad_x = jnp.where(pos < total - 1, ahead - here, 0.0)
    grad_z = jnp.concatenate([here[:, :, 1:] - here[:, :, :-1], jnp.zeros_like(here[:, :, :1])], 2)
    grad_y = jnp.concatenate([here[..., 1:] - here[..., :-1], jnp.zeros_like(here[..., :1])], 3)
    moved = [dual_step * grad for grad in (grad_z, grad_y, grad_x)]
    if duals is not None:
        moved = [dual + step for dual, step in zip(duals, moved)]
    magnitude = jnp.sqrt(sum(jnp.sum(w * w, 1, keepdims=True) for w in moved))
    factor = 1.0 / jnp.maximum(1.0, magnitude / tv_weight)
    duals = [w * factor for w in moved]
    dual_z, dual_y = duals[0][1:], duals[1][1:]
    dual_x = jnp.where(pos < 0, 0.0, duals[2])
    spread_x = dual_x[:-1] - dual_x[1:]
    spread_z = jnp.concatenate([jnp.zeros_like(dual_z[:, :, :1]), dual_z[:, :, :-1]], 2) - dual_z
    spread_y = jnp.concatenate([jnp.zeros_like(dual_y[..., :1]), dual_y[..., :-1]], 3) - dual_y
    return duals, spread_z + spread_y + spread_x


def by_planes(kspace_data, coil_maps, sample_mask, initial_image):
    slabs = lax.axis_size("slab")
    groups = lax.axis_size("coil")
    devices = slabs * groups
    coils, _, depth, ny, nx = coil_maps.shape
    nz, shares = kspace_data.shape[2:4]
    rows = initial_image.shape[2]
    width = nx // devices
    me = lax.axis_index(EVERY)
    forward_y, inverse_y = dft_table(ny, False), dft_table(ny, True)
    forward_z, inverse_z = dft_table(nz, False), dft_table(nz, True)
    inverse_x = jnp.asarray(dft_table(nx, True))
    tables = (on_right(forward_y), on_left(forward_z), on_left(inverse_z), on_right(inverse_y))
    few = max(1, coils // 8)
    hold = lax.optimization_barrier

    def packed(array):
        return array.reshape((devices, width) + array.shape[1:])

    def sent(array):
        return swap(array).reshape((slabs, groups) + array.shape[1:])

    def in_place(array):
        order = Layout(major_to_minor=tuple(range(array.ndim)))
        return with_layout_constraint(array, order)

    first_maps = packed(coil_maps[:few].transpose(4, 0, 1, 2, 3))
    later_maps = packed(coil_maps[few:].transpose(4, 0, 1, 2, 3))
    image = initial_image.reshape(-1, nx).astype(bf16).T.reshape(devices, width, -1)
    edge = jnp.zeros_like(image[:1, :1])
    image = jnp.concatenate(
        [
            jnp.concatenate([edge, image[:-1, -1:]], 0),
            image,
            jnp.concatenate([image[1:, :1], edge], 0),
        ],
        1,
    )
    joined = jnp.concatenate(
        [first_maps.reshape(devices, -1, ny), image.reshape(devices, -1, ny)], 1
    )
    joined = swap(joined)
    mask = shared(sample_mask.swapaxes(1, 2).astype(bf16), slabs)
    joined, mask, later_maps = hold((joined, mask, later_maps))
    later_maps = sent(later_maps)

    image = joined[:, -image.shape[1] * image.shape[2] // ny :]
    first_maps = joined[:, : joined.shape[1] - image.shape[1]]
    first_maps = first_maps.reshape(slabs, groups, width, few, 2, depth, ny)
    image = image.reshape(slabs, groups, width + 2, 2, depth, rows)
    image = image.transpose(2, 3, 0, 4, 1, 5).reshape(width + 2, 2, nz, ny).astype(f32)
    own = image[1:-1]

    data = kspace_data * sample_mask[:, None, :, :, None].astype(bf16)
    data = jnp.einsum("ckzyx,kjxw->wcjyz", data, inverse_x, preferred_element_type=f32)
    data = in_place(data.astype(bf16))
    half = shares // 2
    small = half == SUBLANES and nz == LANES
    if small:
        sampled = sample_mask.swapaxes(1, 2)
        rank = ranks(sampled)
        begin = rank[:, :half, -1:]
        kz = lax.broadcasted_iota(jnp.int32, (1, 1, nz), 2)
        slot = jnp.where(sampled > 0, rank, 0)
        slot = jnp.concatenate([slot[:, :half], jnp.where(sampled[:, half:] > 0, begin + slot[:, half:], 0)], 2)
        spot = jnp.arange(2 * nz, dtype=jnp.int32)
        pick = jnp.sum(
            jnp.where(slot[:, :, None, :] == 1 + kz[..., None], spot, 0), 3, dtype=jnp.int32
        )
        lines = selected(data, pick)
        data, lines, mask = hold((data, lines, mask))
    else:
        data, mask = hold((data, mask))
    mask = mask.swapaxes(0, 1).reshape(coils, slabs * shares, nz)
    masks = []
    for part in (mask[: coils // 2], mask[coils // 2 :]):
        if masks:
            part, _ = hold((part, masks[0]))
        masks.append(lax.all_gather(part, "coil", axis=0))
    mask = jnp.concatenate(masks, 1)

    inverse = (on_right(inverse_z), on_right(inverse_y))
    if small:
        halves = mask.reshape(groups, coils, slabs, 2, half, nz).swapaxes(2, 3)
        rank = ranks(halves)
        begin = rank[:, :, :1, ..., -1:]
        fits = jnp.max(begin + rank[:, :, 1:, ..., -1:]) <= nz
        rank = jnp.concatenate([rank[:, :, :1], begin + rank[:, :, 1:]], 2)
        code = jnp.where(halves > 0, rank - 1, -1).reshape(groups, coils, ny, nz)
        order = np.arange(ny).reshape(slabs, 2, half).swapaxes(0, 1).reshape(-1)
        sparse_inverse = (inverse[0], inverse[1].reshape(2, ny, -1)[:, order].reshape(2 * ny, -1))
    mask = mask.swapaxes(2, 3)
    duals, spread = tv_planes(image, None, me * width, nx)
    normal = normal_of(own, first_maps, mask, 0, tables)
    held = (first_maps, later_maps, mask, data, duals, spread, normal)
    if small:
        (first_maps, later_maps, mask, data, duals, spread, normal), lines, code = hold(
            (held, lines, code)
        )
    else:
        first_maps, later_maps, mask, data, duals, spread, normal = hold(held)

    def finish(data, code, steps, inverse):
        data = [packed(data[:, a:b]) for a, b in steps]
        data = hold(data)
        more = normal_of(own, later_maps, mask, few, tables)
        back = ready = None
        for piece, (a, b) in enumerate(steps):
            got = sent(data[piece])
            rest = data[piece + 1 :]
            if ready is None:
                got, more, rest = hold((got, more, rest))
            else:
                back = ready if back is None else back + ready
                got, back, rest = hold((got, back, rest))
            data[piece + 1 :] = rest
            maps, start = (first_maps, a) if b <= few else (later_maps, a - few)
            codes = None if code is None else (code, a)
            ready = back_of(got, codes, maps, inverse, own.shape, start)
        return more, ready if back is None else back + ready

    def dense(_):
        return finish(data, None, [(few, coils), (0, few)], inverse)

    def sparse(_):
        middle = few + (coils - few + 1) // 2
        steps = [(few, middle), (middle, coils), (0, few)]
        return finish(lines, code, steps, sparse_inverse)

    more, back = lax.cond(fits, sparse, dense, 0) if small else dense(0)
    normal = normal + more
    maps = [(first_maps, 0), (later_maps, few)]
    scale = dual_step / (1.0 + dual_step)
    data_grad = scale * (normal - back)
    change = -primal_step * (data_grad + spread)
    guess = own + 2.0 * change
    line = [g * slabs + s for s in range(slabs) for g in range(groups)]
    before = lax.ppermute(guess[-1:], ("coil", "slab"), list(zip(line[:-1], line[1:])))
    after = lax.ppermute(guess[:1], ("coil", "slab"), list(zip(line[1:], line[:-1])))
    normal = sum(normal_of(guess, m, mask, a, tables) for m, a in maps)
    _, spread = tv_planes(jnp.concatenate([before, guess, after], 0), duals, me * width, nx)
    data_grad = data_grad / (1.0 + dual_step) + scale * (normal - back)
    final = (own + change - primal_step * (data_grad + spread)).astype(bf16)
    final = final.reshape(width, 2, slabs, depth, groups, rows).transpose(2, 4, 0, 1, 3, 5)
    final = swap(final.reshape(devices, -1)).reshape(nx, -1).T
    return final.reshape(initial_image.shape).astype(f32)


def solution(mesh):
    placed = (
        P("coil", None, None, "slab", None),
        P("coil", None, "slab", None, None),
        P("coil", None, "slab"),
        P(None, "slab", "coil", None),
    )

    def on_each(kspace_data, coil_maps, sample_mask, initial_image):
        whole_planes = coil_maps.shape[4] % mesh.size == 0
        form = by_planes if whole_planes else on_device
        return form(kspace_data, coil_maps, sample_mask, initial_image)

    return jax.shard_map(
        on_each,
        mesh=mesh,
        in_specs=placed,
        out_specs=P(None, "slab", "coil", None),
        check_vma=False,
    )
```

```python
import functools
import math

import jax
import jax.numpy as jnp
import ml_dtypes
import numpy as np
from jax import lax
from jax.experimental import pallas as pl
from jax.experimental.layout import Layout, with_layout_constraint
from jax.experimental.pallas import tpu as pltpu
from jax.sharding import PartitionSpec as P

ITERS = 2

dual_step = 0.25
primal_step = 0.25
tv_weight = 0.5
f32 = jnp.float32
bf16 = jnp.bfloat16


def from_behind(block, axis, distance):
    devices = range(lax.axis_size(axis))
    route = [(i - distance, i) for i in devices if i - distance in devices]
    return lax.ppermute(block, axis, route)


def dft_table(length, inverse):
    counter = np.arange(length)
    phase = 2.0 * math.pi / length * (np.outer(counter, counter) % length)
    real_part = np.cos(phase) / math.sqrt(length)
    imag_part = np.sin(phase) / math.sqrt(length)
    if not inverse:
        imag_part = -imag_part
    table = np.stack([np.stack([real_part, imag_part]), np.stack([-imag_part, real_part])])
    return table.astype(ml_dtypes.bfloat16)


def on_right(table):
    n = table.shape[2]
    return jnp.asarray(table.transpose(0, 2, 1, 3).reshape(2 * n, 2 * n))


def on_left(table):
    n = table.shape[2]
    return jnp.asarray(table.transpose(1, 3, 0, 2).reshape(2 * n, 2 * n))


def plane(ref, coil, part):
    block = ref[:, coil, 0, part]
    return block.reshape(block.shape[0] * block.shape[1], block.shape[2])


def dot(a, b, dims=((1,), (0,))):
    return lax.dot_general(a, b, (dims, ((), ())), preferred_element_type=f32)


def combine(out_ref, maps_ref, images, group):
    nz, ny = out_ref.shape[2:]
    real_sum = imag_sum = None
    for coil in range(group):
        real = images[coil * nz : (coil + 1) * nz, :ny]
        imag = images[coil * nz : (coil + 1) * nz, ny:]
        maps_real = plane(maps_ref, coil, 0).astype(f32)
        maps_imag = plane(maps_ref, coil, 1).astype(f32)
        real_term = maps_real * real + maps_imag * imag
        imag_term = maps_real * imag - maps_imag * real
        real_sum = real_term if coil == 0 else real_sum + real_term
        imag_sum = imag_term if coil == 0 else imag_sum + imag_term

    @pl.when(pl.program_id(1) == 0)
    def _():
        out_ref[0, 0] = real_sum
        out_ref[0, 1] = imag_sum

    @pl.when(pl.program_id(1) > 0)
    def _():
        out_ref[0, 0] += real_sum
        out_ref[0, 1] += imag_sum


def normal_kernel(group, guess_ref, maps_ref, mask_ref, fy_ref, fz_ref, gz_ref, gy_ref, out_ref):
    nz, ny = out_ref.shape[2:]
    guess_real = guess_ref[0, 0]
    guess_imag = guess_ref[0, 1]
    rows = []
    for coil in range(group):
        maps_real = plane(maps_ref, coil, 0).astype(f32)
        maps_imag = plane(maps_ref, coil, 1).astype(f32)
        real = maps_real * guess_real - maps_imag * guess_imag
        imag = maps_real * guess_imag + maps_imag * guess_real
        rows.append(jnp.concatenate([real.astype(bf16), imag.astype(bf16)], 1))
    pieces = dot(jnp.concatenate(rows, 0), fy_ref[...]).astype(bf16)
    pieces = jnp.concatenate(
        [
            jnp.concatenate(
                [pieces[c * nz : (c + 1) * nz, j * ny : (j + 1) * ny] for c in range(group)], 1
            )
            for j in range(2)
        ],
        0,
    )
    spectrum = dot(fz_ref[...], pieces).astype(bf16)
    mask = jnp.concatenate([mask_ref[c] for c in range(group)], 1)
    spectrum = spectrum * jnp.concatenate([mask, mask], 0)
    pieces = dot(gz_ref[...], spectrum).astype(bf16)
    pieces = jnp.concatenate(
        [
            jnp.concatenate(
                [pieces[j * nz : (j + 1) * nz, c * ny : (c + 1) * ny] for j in range(2)], 1
            )
            for c in range(group)
        ],
        0,
    )
    combine(out_ref, maps_ref, dot(pieces, gy_ref[...]), group)


def data_kernel(group, data_ref, maps_ref, gy_ref, out_ref):
    columns = jnp.concatenate(
        [
            jnp.concatenate([plane(data_ref, c, 0), plane(data_ref, c, 1)], 0)
            for c in range(group)
        ],
        1,
    )
    combine(out_ref, maps_ref, dot(columns, gy_ref[...], ((0,), (0,))), group)


def whole(shape):
    return pl.BlockSpec(shape, lambda x, c: (0,) * len(shape))


def coil_blocks(array, group):
    src, _, _, parts, planes, cols = array.shape
    return pl.BlockSpec((src, group, 1, parts, planes, cols), lambda x, c: (0, c, x, 0, 0, 0))


def call(kernel, group, operands, specs, shape, coils, flops, nbytes):
    return pl.pallas_call(
        functools.partial(kernel, group),
        out_shape=jax.ShapeDtypeStruct(shape, f32),
        grid=(shape[0], coils // group),
        in_specs=specs,
        out_specs=pl.BlockSpec((1,) + shape[1:], lambda x, c: (x, 0, 0, 0)),
        compiler_params=pltpu.CompilerParams(
            dimension_semantics=("arbitrary", "arbitrary"), vmem_limit_bytes=48 * 2**20
        ),
        cost_estimate=pl.CostEstimate(flops=flops, bytes_accessed=nbytes, transcendentals=0),
    )(*operands)


def coil_group(coils):
    return max(g for g in (1, 2, 4) if coils % g == 0)


def apply_normal(guess, maps, mask, tables):
    coils = maps.shape[1]
    group = coil_group(coils)
    shape = guess.shape
    specs = [
        pl.BlockSpec((1,) + shape[1:], lambda x, c: (x, 0, 0, 0)),
        coil_blocks(maps, group),
        pl.BlockSpec((group,) + mask.shape[1:], lambda x, c: (c, 0, 0)),
    ] + [whole(t.shape) for t in tables]
    cells = coils * shape[0] * shape[2] * shape[3]
    return call(
        normal_kernel, group, (guess, maps, mask) + tables, specs, shape, coils, cells * 4096, cells * 4
    )


def apply_data(data, maps, table, shape):
    coils = maps.shape[1]
    group = coil_group(coils)
    specs = [coil_blocks(data, group), coil_blocks(maps, group), whole(table.shape)]
    cells = coils * shape[0] * shape[2] * shape[3]
    return call(data_kernel, group, (data, maps, table), specs, shape, coils, cells * 1024, cells * 8)


def exchange(blocks):
    got = lax.all_to_all(blocks, "slab", split_axis=0, concat_axis=0, tiled=True)
    if got.shape[4] % 16:
        src, coils, width, parts, share, cols = got.shape
        got = got.transpose(1, 2, 3, 0, 4, 5).reshape(1, coils, width, parts, src * share, cols)
    return got


def tv_update(guess, duals):
    width = guess.shape[0]
    size = lax.axis_size("slab") * width
    pos = lax.axis_index("slab") * width + lax.broadcasted_iota(jnp.int32, (width, 1, 1, 1), 0)
    ahead_x = jnp.concatenate([guess[1:], from_behind(guess[:1], "slab", -1)], 0)
    grad_x = jnp.where(pos < size - 1, ahead_x - guess, 0.0)
    grad_z = jnp.concatenate(
        [guess[:, :, 1:] - guess[:, :, :-1], jnp.zeros_like(guess[:, :, :1])], 2
    )
    grad_y = jnp.concatenate([guess[..., 1:] - guess[..., :-1], jnp.zeros_like(guess[..., :1])], 3)
    moved = [dual_step * grad for grad in (grad_z, grad_y, grad_x)]
    if duals is not None:
        moved = [dual + step for dual, step in zip(duals, moved)]
    magnitude = jnp.sqrt(sum(jnp.sum(w * w, 1, keepdims=True) for w in moved))
    factor = 1.0 / jnp.maximum(1.0, magnitude / tv_weight)
    dual_z, dual_y, dual_x = [w * factor for w in moved]
    prior = from_behind(dual_x[-1:], "slab", 1)
    spread_x = jnp.concatenate([prior, dual_x[:-1]], 0) - dual_x
    spread_z = jnp.concatenate([jnp.zeros_like(dual_z[:, :, :1]), dual_z[:, :, :-1]], 2) - dual_z
    spread_y = jnp.concatenate([jnp.zeros_like(dual_y[..., :1]), dual_y[..., :-1]], 3) - dual_y
    return (dual_z, dual_y, dual_x), spread_z + spread_y + spread_x


def on_device(kspace_data, coil_maps, sample_mask, initial_image):
    slabs = lax.axis_size("slab")
    groups = lax.axis_size("coil")
    coils, _, planes, ny, nx = coil_maps.shape
    nz = kspace_data.shape[2]
    shares = kspace_data.shape[3]
    rows = initial_image.shape[2]
    width = nx // slabs
    forward_y, inverse_y = dft_table(ny, False), dft_table(ny, True)
    forward_z, inverse_z = dft_table(nz, False), dft_table(nz, True)
    inverse_x = jnp.asarray(dft_table(nx, True))
    tables = (on_right(forward_y), on_left(forward_z), on_left(inverse_z), on_right(inverse_y))

    image = initial_image.reshape(2, planes, rows, slabs, width).transpose(3, 4, 0, 2, 1)
    image = lax.all_to_all(
        image.reshape(slabs, -1), "slab", split_axis=0, concat_axis=0, tiled=True
    ).reshape(slabs, width, 2, rows, planes)
    image = image.transpose(1, 2, 3, 0, 4).reshape(width, 2, rows, nz)
    image = lax.all_gather(image, "coil", axis=2, tiled=True).swapaxes(2, 3)
    mask = lax.all_gather(sample_mask.astype(bf16), "slab", axis=2, tiled=True)

    maps = coil_maps.reshape(coils, 2, planes, ny, slabs, width).transpose(4, 0, 5, 1, 2, 3)
    maps, image, mask = lax.optimization_barrier((maps, image, mask))
    maps = exchange(maps)

    data = kspace_data * sample_mask[:, None, :, :, None].astype(bf16)
    data = jnp.einsum("ckzyx,kjxw->cjzyw", data, inverse_x, preferred_element_type=f32).astype(bf16)
    data = jnp.einsum(
        "ckzyx,kjzw->cjywx", data, jnp.asarray(inverse_z), preferred_element_type=f32
    ).astype(bf16)
    data = data.reshape(coils, 2, shares, nz, slabs, width).transpose(4, 0, 5, 1, 2, 3)
    data, maps = lax.optimization_barrier((data, maps))
    data = exchange(data)

    normal = apply_normal(image, maps, mask, tables)
    duals, spread = tv_update(image, None)
    data, normal, duals, spread = lax.optimization_barrier((data, normal, duals, spread))
    back_data = apply_data(data, maps, tables[3], image.shape)
    scale = dual_step / (1.0 + dual_step)
    data_grad = lax.psum(scale * (normal - back_data), "coil")
    updated = image - primal_step * (data_grad + spread)
    guess = 2.0 * updated - image
    normal = apply_normal(guess, maps, mask, tables)
    _, spread = tv_update(guess, duals)
    known = updated - primal_step * (data_grad / (1.0 + dual_step) + spread)
    share = known / groups - (primal_step * scale) * (normal - back_data)
    share = lax.psum_scatter(share.swapaxes(2, 3), "coil", scatter_dimension=2, tiled=True)
    share = share.reshape(width, 2, rows, slabs, planes).transpose(3, 1, 4, 2, 0)
    share = lax.all_to_all(
        share.reshape(slabs, -1), "slab", split_axis=0, concat_axis=0, tiled=True
    ).reshape(slabs, 2, planes, rows, width)
    return share.transpose(1, 2, 3, 0, 4).reshape(2, planes, rows, nx)


def all_planes(ref, coil, turn, part):
    block = ref[:, coil, 0, turn, part]
    return block.reshape(block.shape[0] * block.shape[1], block.shape[2])


def terms(maps, images):
    nz, ny = maps[0][0].shape
    real_sum = imag_sum = None
    for coil, (maps_real, maps_imag) in enumerate(maps):
        real = images[coil * nz : (coil + 1) * nz, :ny]
        imag = images[coil * nz : (coil + 1) * nz, ny:]
        real_term = maps_real * real + maps_imag * imag
        imag_term = maps_real * imag - maps_imag * real
        real_sum = real_term if coil == 0 else real_sum + real_term
        imag_sum = imag_term if coil == 0 else imag_sum + imag_term
    return real_sum, imag_sum


def add_up(out_ref, sums):
    real_sum = functools.reduce(lambda a, b: a + b, [real for real, _ in sums])
    imag_sum = functools.reduce(lambda a, b: a + b, [imag for _, imag in sums])

    @pl.when(pl.program_id(1) == 0)
    def _():
        out_ref[0, 0] = real_sum
        out_ref[0, 1] = imag_sum

    @pl.when(pl.program_id(1) > 0)
    def _():
        out_ref[0, 0] += real_sum
        out_ref[0, 1] += imag_sum


def planes_of(maps_ref, turn):
    return [
        (all_planes(maps_ref, c, turn, 0).astype(f32), all_planes(maps_ref, c, turn, 1).astype(f32))
        for c in range(maps_ref.shape[1])
    ]


def normal_planes(guess_ref, maps_ref, mask_ref, fy_ref, fz_ref, gz_ref, gy_ref, out_ref):
    nz, ny = out_ref.shape[2:]
    group = maps_ref.shape[1]
    guess_real = guess_ref[0, 0]
    guess_imag = guess_ref[0, 1]
    sums = []
    for turn in range(maps_ref.shape[3]):
        maps = planes_of(maps_ref, turn)
        rows = []
        for maps_real, maps_imag in maps:
            real = maps_real * guess_real - maps_imag * guess_imag
            imag = maps_real * guess_imag + maps_imag * guess_real
            rows.append(jnp.concatenate([real.astype(bf16), imag.astype(bf16)], 1))
        pieces = dot(jnp.concatenate(rows, 0), fy_ref[...]).astype(bf16)
        pieces = jnp.concatenate(
            [
                jnp.concatenate(
                    [pieces[c * nz : (c + 1) * nz, j * ny : (j + 1) * ny] for c in range(group)], 1
                )
                for j in range(2)
            ],
            0,
        )
        spectrum = dot(fz_ref[...], pieces).astype(bf16)
        mask = jnp.concatenate([mask_ref[c, turn] for c in range(group)], 1)
        spectrum = spectrum * jnp.concatenate([mask, mask], 0)
        pieces = dot(gz_ref[...], spectrum).astype(bf16)
        pieces = jnp.concatenate(
            [
                jnp.concatenate(
                    [pieces[j * nz : (j + 1) * nz, c * ny : (c + 1) * ny] for j in range(2)], 1
                )
                for c in range(group)
            ],
            0,
        )
        sums.append(terms(maps, dot(pieces, gy_ref[...])))
    add_up(out_ref, sums)


def back_terms(maps_ref, turn, gz_ref, gy_ref, spectra):
    nz = gz_ref.shape[1] // 2
    shares = spectra[0][0].shape[0]
    spectrum = jnp.concatenate([jnp.concatenate(parts, 1) for parts in spectra], 0)
    pieces = dot(spectrum, gz_ref[...]).astype(bf16)
    columns = jnp.concatenate(
        [
            jnp.concatenate(
                [
                    pieces[c * shares : (c + 1) * shares, j * nz : (j + 1) * nz]
                    for c in range(len(spectra))
                ],
                1,
            )
            for j in range(2)
        ],
        0,
    )
    return terms(planes_of(maps_ref, turn), dot(columns, gy_ref[...], ((0,), (0,))))


def dense_kernel(data_ref, maps_ref, gz_ref, gy_ref, out_ref):
    sums = []
    for turn in range(maps_ref.shape[3]):
        spectra = [
            (all_planes(data_ref, c, turn, 0), all_planes(data_ref, c, turn, 1))
            for c in range(data_ref.shape[1])
        ]
        sums.append(back_terms(maps_ref, turn, gz_ref, gy_ref, spectra))
    add_up(out_ref, sums)


def lanes_at(array, place):
    return jnp.take_along_axis(array, place, 1, mode="promise_in_bounds")


def sparse_kernel(data_ref, code_ref, maps_ref, gz_ref, gy_ref, out_ref):
    half = data_ref.shape[4] // 2
    sums = []
    for turn in range(maps_ref.shape[3]):
        spectra = []
        for coil in range(data_ref.shape[1]):
            lines = data_ref[:, coil, 0, turn].astype(f32)
            lines = [
                lines[:, j * half : (j + 1) * half].reshape(-1, lines.shape[2]) for j in range(2)
            ]
            count = lines[0].shape[0]
            codes = [code_ref[coil, turn, h * count : (h + 1) * count] for h in range(2)]
            spectra.append(
                [
                    jnp.concatenate(
                        [
                            jnp.where(code >= 0, lanes_at(line, jnp.maximum(code, 0)), 0.0)
                            for code in codes
                        ],
                        0,
                    ).astype(bf16)
                    for line in lines
                ]
            )
        sums.append(back_terms(maps_ref, turn, gz_ref, gy_ref, spectra))
    add_up(out_ref, sums)


def select_kernel(edges, pick_ref, data_ref, *out_refs):
    half = data_ref.shape[3] // 2
    lanes = data_ref.shape[4]

    def one(plane_index, _):
        for out_ref, (first, last) in zip(out_refs, edges):
            for coil in range(first, last):
                pick = pick_ref[coil]
                later = pick >= lanes
                place = jnp.where(later, pick - lanes, pick)
                parts = []
                for part in range(2):
                    lines = data_ref[plane_index, coil, part].astype(f32)
                    parts.append(
                        jnp.where(
                            later, lanes_at(lines[half:], place), lanes_at(lines[:half], place)
                        )
                    )
                out_ref[plane_index, coil - first] = jnp.concatenate(parts, 0).astype(bf16)
        return 0

    lax.fori_loop(0, data_ref.shape[0], one, 0)


def selected(data, pick, edges):
    planes, _, _, shares, lanes = data.shape
    step = max(n for n in (1, 2, 4, 8) if planes % n == 0)
    return pl.pallas_call(
        functools.partial(select_kernel, edges),
        out_shape=[
            jax.ShapeDtypeStruct((planes, b - a, shares, lanes), bf16) for a, b in edges
        ],
        grid=(planes // step,),
        in_specs=[
            pl.BlockSpec(pick.shape, lambda x: (0, 0, 0)),
            pl.BlockSpec((step,) + data.shape[1:], lambda x: (x, 0, 0, 0, 0)),
        ],
        out_specs=[
            pl.BlockSpec((step, b - a, shares, lanes), lambda x: (x, 0, 0, 0)) for a, b in edges
        ],
        compiler_params=pltpu.CompilerParams(dimension_semantics=("arbitrary",)),
        cost_estimate=pl.CostEstimate(
            flops=data.size * 64, bytes_accessed=data.size * 3, transcendentals=0
        ),
    )(pick, data)


def deliver_kernel(block_ref, got_ref, send_sem, recv_sem):
    groups = lax.axis_size("coil")
    count = groups * lax.axis_size("slab")
    me = lax.axis_index("slab") * groups + lax.axis_index("coil")
    barrier = pltpu.get_barrier_semaphore()

    def place(step):
        other = lax.rem(me + step, count)
        return other, (lax.rem(other, groups), other // groups)

    def greet(step, _):
        pl.semaphore_signal(
            barrier, inc=1, device_id=place(step)[1], device_id_type=pl.DeviceIdType.MESH
        )
        return 0

    def copy(step):
        other, device = place(step)
        return pltpu.make_async_remote_copy(
            block_ref.at[other],
            got_ref.at[me],
            send_sem.at[step - 1],
            recv_sem.at[step - 1],
            device_id=device,
            device_id_type=pl.DeviceIdType.MESH,
        )

    def begin(step, _):
        copy(step).start()
        return 0

    def end(step, _):
        copy(step).wait()
        return 0

    lax.fori_loop(1, count, greet, 0)
    pl.semaphore_wait(barrier, count - 1)
    lax.fori_loop(1, count, begin, 0)
    got_ref[me] = block_ref[me]
    lax.fori_loop(1, count, end, 0)


def delivered(blocks):
    return pl.pallas_call(
        deliver_kernel,
        out_shape=jax.ShapeDtypeStruct(blocks.shape, blocks.dtype),
        in_specs=[pl.BlockSpec(memory_space=pltpu.VMEM)],
        out_specs=pl.BlockSpec(memory_space=pltpu.VMEM),
        scratch_shapes=[
            pltpu.SemaphoreType.DMA((blocks.shape[0] - 1,)),
            pltpu.SemaphoreType.DMA((blocks.shape[0] - 1,)),
        ],
        compiler_params=pltpu.CompilerParams(collective_id=1, has_side_effects=True),
        cost_estimate=pl.CostEstimate(
            flops=blocks.size * 64, bytes_accessed=blocks.size * 4, transcendentals=0
        ),
    )(blocks)


def share_kernel(own_ref, all_ref, send_sem, recv_sem):
    count = lax.axis_size("slab")
    slab, coil = lax.axis_index("slab"), lax.axis_index("coil")

    def device(step):
        return (coil, lax.rem(slab + step, count))

    barrier = pltpu.get_barrier_semaphore()
    for step in range(1, count):
        pl.semaphore_signal(
            barrier, inc=1, device_id=device(step), device_id_type=pl.DeviceIdType.MESH
        )
    pl.semaphore_wait(barrier, count - 1)
    copies = [
        pltpu.make_async_remote_copy(
            own_ref,
            all_ref.at[slab],
            send_sem.at[step - 1],
            recv_sem.at[step - 1],
            device_id=device(step),
            device_id_type=pl.DeviceIdType.MESH,
        )
        for step in range(1, count)
    ]
    for copy in copies:
        copy.start()
    all_ref[slab] = own_ref[...]
    for copy in copies:
        copy.wait()


def shared(own, slabs):
    return pl.pallas_call(
        share_kernel,
        out_shape=jax.ShapeDtypeStruct((slabs,) + own.shape, own.dtype),
        in_specs=[pl.BlockSpec(memory_space=pltpu.VMEM)],
        out_specs=pl.BlockSpec(memory_space=pltpu.VMEM),
        scratch_shapes=[
            pltpu.SemaphoreType.DMA((slabs - 1,)),
            pltpu.SemaphoreType.DMA((slabs - 1,)),
        ],
        compiler_params=pltpu.CompilerParams(collective_id=0, has_side_effects=True),
        cost_estimate=pl.CostEstimate(
            flops=own.size * 64, bytes_accessed=own.size * 32, transcendentals=0
        ),
    )(own)


def plane_call(kernel, operands, specs, shape, steps, flops, nbytes):
    return pl.pallas_call(
        kernel,
        out_shape=jax.ShapeDtypeStruct(shape, f32),
        grid=(shape[0], steps),
        in_specs=specs,
        out_specs=pl.BlockSpec((1,) + shape[1:], lambda x, c: (x, 0, 0, 0)),
        compiler_params=pltpu.CompilerParams(
            dimension_semantics=("arbitrary", "arbitrary"), vmem_limit_bytes=48 * 2**20
        ),
        cost_estimate=pl.CostEstimate(flops=flops, bytes_accessed=nbytes, transcendentals=0),
    )(*operands)


def every_source(array, turns, start=0):
    slabs, groups, _, _, *rest = array.shape
    return pl.BlockSpec(
        (slabs, groups, 1, turns, *rest),
        lambda x, c: (0, 0, x, start + c) + (0,) * len(rest),
    )


def per_coil(array, turns, start=0):
    return pl.BlockSpec(
        (array.shape[0], turns) + array.shape[2:], lambda x, c: (0, start + c, 0, 0)
    )


def normal_of(guess, maps, mask, tables):
    shape = guess.shape
    groups, coils = maps.shape[1], maps.shape[3]
    turns = math.gcd(coils, 4)
    specs = [
        pl.BlockSpec((1,) + shape[1:], lambda x, c: (x, 0, 0, 0)),
        every_source(maps, turns),
        per_coil(mask, turns),
    ] + [whole(t.shape) for t in tables]
    cells = groups * coils * shape[0] * shape[2] * shape[3]
    operands = (guess, maps, mask) + tables
    steps = coils // turns
    return plane_call(normal_planes, operands, specs, shape, steps, cells * 4096, cells * 4)


def back_of(data, code, maps, tables, shape, start):
    groups, coils = maps.shape[1], data.shape[3]
    turns = math.gcd(math.gcd(coils, start), 2)
    steps, start = coils // turns, start // turns
    operands, specs = [data], [every_source(data, turns)]
    if code is not None:
        operands.append(code)
        specs.append(per_coil(code, turns, start))
    operands += (maps,) + tables
    specs += [every_source(maps, turns, start)] + [whole(t.shape) for t in tables]
    cells = groups * coils * shape[0] * shape[2] * shape[3]
    kernel = dense_kernel if code is None else sparse_kernel
    return plane_call(kernel, operands, specs, shape, steps, cells * 2048, cells * 8)


EVERY = ("slab", "coil")
LANES = 128
SUBLANES = 8


def ranks(flags):
    size = flags.shape[-1]
    flags = flags.astype(bf16)

    def count(table):
        sums = jnp.einsum("...k,kl->...l", flags, table, preferred_element_type=f32)
        return sums.astype(jnp.int32)

    every = jnp.ones((size, size), bf16)
    return count(jnp.triu(every)), count(every)


def swap(blocks):
    return lax.all_to_all(blocks, EVERY, split_axis=0, concat_axis=0, tiled=True)


def tv_planes(guess, duals, first, total):
    here, ahead = guess[:-1], guess[1:]
    pos = first - 1 + lax.broadcasted_iota(jnp.int32, (here.shape[0], 1, 1, 1), 0)
    grad_x = jnp.where(pos < total - 1, ahead - here, 0.0)
    grad_z = jnp.concatenate([here[:, :, 1:] - here[:, :, :-1], jnp.zeros_like(here[:, :, :1])], 2)
    grad_y = jnp.concatenate([here[..., 1:] - here[..., :-1], jnp.zeros_like(here[..., :1])], 3)
    moved = [dual_step * grad for grad in (grad_z, grad_y, grad_x)]
    if duals is not None:
        moved = [dual + step for dual, step in zip(duals, moved)]
    magnitude = jnp.sqrt(sum(jnp.sum(w * w, 1, keepdims=True) for w in moved))
    factor = 1.0 / jnp.maximum(1.0, magnitude / tv_weight)
    duals = [w * factor for w in moved]
    dual_z, dual_y = duals[0][1:], duals[1][1:]
    dual_x = jnp.where(pos < 0, 0.0, duals[2])
    spread_x = dual_x[:-1] - dual_x[1:]
    spread_z = jnp.concatenate([jnp.zeros_like(dual_z[:, :, :1]), dual_z[:, :, :-1]], 2) - dual_z
    spread_y = jnp.concatenate([jnp.zeros_like(dual_y[..., :1]), dual_y[..., :-1]], 3) - dual_y
    return duals, spread_z + spread_y + spread_x


def by_planes(kspace_data, coil_maps, sample_mask, initial_image):
    slabs = lax.axis_size("slab")
    groups = lax.axis_size("coil")
    devices = slabs * groups
    coils, _, depth, ny, nx = coil_maps.shape
    nz, shares = kspace_data.shape[2:4]
    rows = initial_image.shape[2]
    width = nx // devices
    me = lax.axis_index(EVERY)
    forward_y, inverse_y = dft_table(ny, False), dft_table(ny, True)
    forward_z, inverse_z = dft_table(nz, False), dft_table(nz, True)
    inverse_x = jnp.asarray(dft_table(nx, True))
    tables = (on_right(forward_y), on_left(forward_z), on_left(inverse_z), on_right(inverse_y))
    hold = lax.optimization_barrier

    def packed(array):
        return array.reshape((devices, width) + array.shape[1:])

    def sent(array):
        return swap(array).reshape((slabs, groups) + array.shape[1:])

    def in_place(array):
        order = Layout(major_to_minor=tuple(range(array.ndim)))
        return with_layout_constraint(array, order)

    image = initial_image.reshape(-1, nx).astype(bf16).T.reshape(devices, width, -1)
    edge = jnp.zeros_like(image[:1, :1])
    image = jnp.concatenate(
        [
            jnp.concatenate([edge, image[:-1, -1:]], 0),
            image,
            jnp.concatenate([image[1:, :1], edge], 0),
        ],
        1,
    )
    image = image.reshape(devices, -1, ny)
    image, coil_maps = hold((image, coil_maps))
    image = swap(image)
    mask = shared(sample_mask.swapaxes(1, 2).astype(bf16), slabs)
    maps = packed(coil_maps.transpose(4, 0, 1, 2, 3))
    image, mask, maps = hold((image, mask, maps))
    maps = sent(maps)

    image = image.reshape(slabs, groups, width + 2, 2, depth, rows)
    image = image.transpose(2, 3, 0, 4, 1, 5).reshape(width + 2, 2, nz, ny)
    image = hold(image).astype(f32)
    own = image[1:-1]

    data = kspace_data * sample_mask[:, None, :, :, None].astype(bf16)
    data = jnp.einsum("ckzyx,kjxw->wcjyz", data, inverse_x, preferred_element_type=f32)
    data = in_place(data.astype(bf16))
    half = shares // 2
    small = half == SUBLANES and nz == LANES
    last = max(1, coils // 4)
    edges = [(0, coils - last), (coils - last, coils)]
    if small:
        sampled = sample_mask.swapaxes(1, 2)
        rank, total = ranks(sampled)
        begin = total[:, :half]
        kz = lax.broadcasted_iota(jnp.int32, (1, 1, nz), 2)
        slot = jnp.where(sampled > 0, rank, 0)
        second = jnp.where(sampled[:, half:] > 0, begin + slot[:, half:], 0)
        slot = jnp.concatenate([slot[:, :half], second], 2)
        spot = jnp.arange(2 * nz, dtype=jnp.int32)
        pick = jnp.sum(
            jnp.where(slot[:, :, None, :] == 1 + kz[..., None], spot, 0), 3, dtype=jnp.int32
        )
        lines = [packed(piece) for piece in selected(data, pick, edges)]
        data, lines, mask = hold((data, lines, mask))
    else:
        data, mask = hold((data, mask))
    mask = mask.swapaxes(0, 1).reshape(coils, slabs * shares, nz)
    masks = []
    for part in (mask[: coils // 2], mask[coils // 2 :]):
        if masks:
            part, _ = hold((part, masks[0]))
        masks.append(lax.all_gather(part, "coil", axis=0))
    mask = jnp.concatenate(masks, 1)

    inverse = (on_right(inverse_z), on_right(inverse_y))
    if small:
        halves = hold(mask.reshape(groups, coils, slabs, 2, half, nz).swapaxes(2, 3))
        rank, total = ranks(halves)
        begin = total[:, :, :1]
        fits = jnp.max(begin + total[:, :, 1:]) <= nz
        rank = jnp.concatenate([rank[:, :, :1], begin + rank[:, :, 1:]], 2)
        code = jnp.where(halves > 0, rank - 1, -1).reshape(groups, coils, ny, nz)
        order = np.arange(ny).reshape(slabs, 2, half).swapaxes(0, 1).reshape(-1)
        sparse_inverse = (inverse[0], inverse[1].reshape(2, ny, -1)[:, order].reshape(2 * ny, -1))
    mask = mask.swapaxes(2, 3)
    duals, spread = tv_planes(image, None, me * width, nx)
    held = (maps, mask, data, own, duals, spread)
    if small:
        (maps, mask, data, own, duals, spread), lines, code = hold((held, lines, code))
    else:
        maps, mask, data, own, duals, spread = hold(held)

    def finish(pieces, code, inverse):
        normal = normal_of(own, maps, mask, tables)
        back, start = None, 0
        for turn in range(len(pieces)):
            got = sent(pieces[turn])
            if turn == 0:
                got, normal, pieces = hold((got, normal, pieces))
            term = back_of(got, code, maps, inverse, own.shape, start)
            back = term if back is None else back + term
            start += got.shape[3]
        return normal, back

    def dense(_):
        return finish([packed(data)], None, inverse)

    def sparse(_):
        return finish(lines, code, sparse_inverse)

    normal, back = lax.cond(fits, sparse, dense, 0) if small else dense(0)
    scale = dual_step / (1.0 + dual_step)
    data_grad = scale * (normal - back)
    change = -primal_step * (data_grad + spread)
    guess = own + 2.0 * change
    line = [g * slabs + s for s in range(slabs) for g in range(groups)]
    before = lax.ppermute(guess[-1:], ("coil", "slab"), list(zip(line[:-1], line[1:])))
    after = lax.ppermute(guess[:1], ("coil", "slab"), list(zip(line[1:], line[:-1])))
    normal = normal_of(guess, maps, mask, tables)
    _, spread = tv_planes(jnp.concatenate([before, guess, after], 0), duals, me * width, nx)
    data_grad = data_grad / (1.0 + dual_step) + scale * (normal - back)
    final = (own + change - primal_step * (data_grad + spread)).astype(bf16)
    final = final.reshape(width, 2, slabs, depth, groups, rows).transpose(2, 4, 0, 1, 3, 5)
    final = delivered(final.reshape(devices, -1, LANES)).reshape(nx, -1).T
    return final.reshape(initial_image.shape).astype(f32)


def solution(mesh):
    placed = (
        P("coil", None, None, "slab", None),
        P("coil", None, "slab", None, None),
        P("coil", None, "slab"),
        P(None, "slab", "coil", None),
    )

    def on_each(kspace_data, coil_maps, sample_mask, initial_image):
        whole_planes = coil_maps.shape[4] % mesh.size == 0
        form = by_planes if whole_planes else on_device
        return form(kspace_data, coil_maps, sample_mask, initial_image)

    return jax.shard_map(
        on_each,
        mesh=mesh,
        in_specs=placed,
        out_specs=P(None, "slab", "coil", None),
        check_vma=False,
    )
```

```python
import functools
import math

import jax
import jax.numpy as jnp
import ml_dtypes
import numpy as np
from jax import lax
from jax.experimental import pallas as pl
from jax.experimental.layout import Layout, with_layout_constraint
from jax.experimental.pallas import tpu as pltpu
from jax.sharding import PartitionSpec as P


dual_step = 0.25
primal_step = 0.25
tv_weight = 0.5
f32 = jnp.float32
bf16 = jnp.bfloat16


def from_behind(block, axis, distance):
    devices = range(lax.axis_size(axis))
    route = [(i - distance, i) for i in devices if i - distance in devices]
    return lax.ppermute(block, axis, route)


def dft_table(length, inverse):
    counter = np.arange(length)
    phase = 2.0 * math.pi / length * (np.outer(counter, counter) % length)
    real_part = np.cos(phase) / math.sqrt(length)
    imag_part = np.sin(phase) / math.sqrt(length)
    if not inverse:
        imag_part = -imag_part
    table = np.stack([np.stack([real_part, imag_part]), np.stack([-imag_part, real_part])])
    return table.astype(ml_dtypes.bfloat16)


def on_right(table):
    n = table.shape[2]
    return jnp.asarray(table.transpose(0, 2, 1, 3).reshape(2 * n, 2 * n))


def on_left(table):
    n = table.shape[2]
    return jnp.asarray(table.transpose(1, 3, 0, 2).reshape(2 * n, 2 * n))


def plane(ref, coil, part):
    block = ref[:, coil, 0, part]
    return block.reshape(block.shape[0] * block.shape[1], block.shape[2])


def dot(a, b, dims=((1,), (0,))):
    return lax.dot_general(a, b, (dims, ((), ())), preferred_element_type=f32)


def combine(out_ref, maps_ref, images, group):
    nz, ny = out_ref.shape[2:]
    real_sum = imag_sum = None
    for coil in range(group):
        real = images[coil * nz : (coil + 1) * nz, :ny]
        imag = images[coil * nz : (coil + 1) * nz, ny:]
        maps_real = plane(maps_ref, coil, 0).astype(f32)
        maps_imag = plane(maps_ref, coil, 1).astype(f32)
        real_term = maps_real * real + maps_imag * imag
        imag_term = maps_real * imag - maps_imag * real
        real_sum = real_term if coil == 0 else real_sum + real_term
        imag_sum = imag_term if coil == 0 else imag_sum + imag_term

    @pl.when(pl.program_id(1) == 0)
    def _():
        out_ref[0, 0] = real_sum
        out_ref[0, 1] = imag_sum

    @pl.when(pl.program_id(1) > 0)
    def _():
        out_ref[0, 0] += real_sum
        out_ref[0, 1] += imag_sum


def normal_kernel(group, guess_ref, maps_ref, mask_ref, fy_ref, fz_ref, gz_ref, gy_ref, out_ref):
    nz, ny = out_ref.shape[2:]
    guess_real = guess_ref[0, 0]
    guess_imag = guess_ref[0, 1]
    rows = []
    for coil in range(group):
        maps_real = plane(maps_ref, coil, 0).astype(f32)
        maps_imag = plane(maps_ref, coil, 1).astype(f32)
        real = maps_real * guess_real - maps_imag * guess_imag
        imag = maps_real * guess_imag + maps_imag * guess_real
        rows.append(jnp.concatenate([real.astype(bf16), imag.astype(bf16)], 1))
    pieces = dot(jnp.concatenate(rows, 0), fy_ref[...]).astype(bf16)
    pieces = jnp.concatenate(
        [
            jnp.concatenate(
                [pieces[c * nz : (c + 1) * nz, j * ny : (j + 1) * ny] for c in range(group)], 1
            )
            for j in range(2)
        ],
        0,
    )
    spectrum = dot(fz_ref[...], pieces).astype(bf16)
    mask = jnp.concatenate([mask_ref[c] for c in range(group)], 1)
    spectrum = spectrum * jnp.concatenate([mask, mask], 0)
    pieces = dot(gz_ref[...], spectrum).astype(bf16)
    pieces = jnp.concatenate(
        [
            jnp.concatenate(
                [pieces[j * nz : (j + 1) * nz, c * ny : (c + 1) * ny] for j in range(2)], 1
            )
            for c in range(group)
        ],
        0,
    )
    combine(out_ref, maps_ref, dot(pieces, gy_ref[...]), group)


def data_kernel(group, data_ref, maps_ref, gy_ref, out_ref):
    columns = jnp.concatenate(
        [
            jnp.concatenate([plane(data_ref, c, 0), plane(data_ref, c, 1)], 0)
            for c in range(group)
        ],
        1,
    )
    combine(out_ref, maps_ref, dot(columns, gy_ref[...], ((0,), (0,))), group)


def whole(shape):
    return pl.BlockSpec(shape, lambda x, c: (0,) * len(shape))


def coil_blocks(array, group):
    src, _, _, parts, planes, cols = array.shape
    return pl.BlockSpec((src, group, 1, parts, planes, cols), lambda x, c: (0, c, x, 0, 0, 0))


def call(kernel, group, operands, specs, shape, coils, flops, nbytes):
    return pl.pallas_call(
        functools.partial(kernel, group),
        out_shape=jax.ShapeDtypeStruct(shape, f32),
        grid=(shape[0], coils // group),
        in_specs=specs,
        out_specs=pl.BlockSpec((1,) + shape[1:], lambda x, c: (x, 0, 0, 0)),
        compiler_params=pltpu.CompilerParams(
            dimension_semantics=("arbitrary", "arbitrary"), vmem_limit_bytes=48 * 2**20
        ),
        cost_estimate=pl.CostEstimate(flops=flops, bytes_accessed=nbytes, transcendentals=0),
    )(*operands)


def coil_group(coils):
    return max(g for g in (1, 2, 4) if coils % g == 0)


def apply_normal(guess, maps, mask, tables):
    coils = maps.shape[1]
    group = coil_group(coils)
    shape = guess.shape
    specs = [
        pl.BlockSpec((1,) + shape[1:], lambda x, c: (x, 0, 0, 0)),
        coil_blocks(maps, group),
        pl.BlockSpec((group,) + mask.shape[1:], lambda x, c: (c, 0, 0)),
    ] + [whole(t.shape) for t in tables]
    cells = coils * shape[0] * shape[2] * shape[3]
    return call(
        normal_kernel, group, (guess, maps, mask) + tables, specs, shape, coils, cells * 4096, cells * 4
    )


def apply_data(data, maps, table, shape):
    coils = maps.shape[1]
    group = coil_group(coils)
    specs = [coil_blocks(data, group), coil_blocks(maps, group), whole(table.shape)]
    cells = coils * shape[0] * shape[2] * shape[3]
    return call(data_kernel, group, (data, maps, table), specs, shape, coils, cells * 1024, cells * 8)


def exchange(blocks):
    got = lax.all_to_all(blocks, "slab", split_axis=0, concat_axis=0, tiled=True)
    if got.shape[4] % 16:
        src, coils, width, parts, share, cols = got.shape
        got = got.transpose(1, 2, 3, 0, 4, 5).reshape(1, coils, width, parts, src * share, cols)
    return got


def tv_update(guess, duals):
    width = guess.shape[0]
    size = lax.axis_size("slab") * width
    pos = lax.axis_index("slab") * width + lax.broadcasted_iota(jnp.int32, (width, 1, 1, 1), 0)
    ahead_x = jnp.concatenate([guess[1:], from_behind(guess[:1], "slab", -1)], 0)
    grad_x = jnp.where(pos < size - 1, ahead_x - guess, 0.0)
    grad_z = jnp.concatenate(
        [guess[:, :, 1:] - guess[:, :, :-1], jnp.zeros_like(guess[:, :, :1])], 2
    )
    grad_y = jnp.concatenate([guess[..., 1:] - guess[..., :-1], jnp.zeros_like(guess[..., :1])], 3)
    moved = [dual_step * grad for grad in (grad_z, grad_y, grad_x)]
    if duals is not None:
        moved = [dual + step for dual, step in zip(duals, moved)]
    magnitude = jnp.sqrt(sum(jnp.sum(w * w, 1, keepdims=True) for w in moved))
    factor = 1.0 / jnp.maximum(1.0, magnitude / tv_weight)
    dual_z, dual_y, dual_x = [w * factor for w in moved]
    prior = from_behind(dual_x[-1:], "slab", 1)
    spread_x = jnp.concatenate([prior, dual_x[:-1]], 0) - dual_x
    spread_z = jnp.concatenate([jnp.zeros_like(dual_z[:, :, :1]), dual_z[:, :, :-1]], 2) - dual_z
    spread_y = jnp.concatenate([jnp.zeros_like(dual_y[..., :1]), dual_y[..., :-1]], 3) - dual_y
    return (dual_z, dual_y, dual_x), spread_z + spread_y + spread_x


def on_device(kspace_data, coil_maps, sample_mask, initial_image):
    slabs = lax.axis_size("slab")
    groups = lax.axis_size("coil")
    coils, _, planes, ny, nx = coil_maps.shape
    nz = kspace_data.shape[2]
    shares = kspace_data.shape[3]
    rows = initial_image.shape[2]
    width = nx // slabs
    forward_y, inverse_y = dft_table(ny, False), dft_table(ny, True)
    forward_z, inverse_z = dft_table(nz, False), dft_table(nz, True)
    inverse_x = jnp.asarray(dft_table(nx, True))
    tables = (on_right(forward_y), on_left(forward_z), on_left(inverse_z), on_right(inverse_y))

    image = initial_image.reshape(2, planes, rows, slabs, width).transpose(3, 4, 0, 2, 1)
    image = lax.all_to_all(
        image.reshape(slabs, -1), "slab", split_axis=0, concat_axis=0, tiled=True
    ).reshape(slabs, width, 2, rows, planes)
    image = image.transpose(1, 2, 3, 0, 4).reshape(width, 2, rows, nz)
    image = lax.all_gather(image, "coil", axis=2, tiled=True).swapaxes(2, 3)
    mask = lax.all_gather(sample_mask.astype(bf16), "slab", axis=2, tiled=True)

    maps = coil_maps.reshape(coils, 2, planes, ny, slabs, width).transpose(4, 0, 5, 1, 2, 3)
    maps, image, mask = lax.optimization_barrier((maps, image, mask))
    maps = exchange(maps)

    data = kspace_data * sample_mask[:, None, :, :, None].astype(bf16)
    data = jnp.einsum("ckzyx,kjxw->cjzyw", data, inverse_x, preferred_element_type=f32).astype(bf16)
    data = jnp.einsum(
        "ckzyx,kjzw->cjywx", data, jnp.asarray(inverse_z), preferred_element_type=f32
    ).astype(bf16)
    data = data.reshape(coils, 2, shares, nz, slabs, width).transpose(4, 0, 5, 1, 2, 3)
    data, maps = lax.optimization_barrier((data, maps))
    data = exchange(data)

    normal = apply_normal(image, maps, mask, tables)
    duals, spread = tv_update(image, None)
    data, normal, duals, spread = lax.optimization_barrier((data, normal, duals, spread))
    back_data = apply_data(data, maps, tables[3], image.shape)
    scale = dual_step / (1.0 + dual_step)
    data_grad = lax.psum(scale * (normal - back_data), "coil")
    updated = image - primal_step * (data_grad + spread)
    guess = 2.0 * updated - image
    normal = apply_normal(guess, maps, mask, tables)
    _, spread = tv_update(guess, duals)
    known = updated - primal_step * (data_grad / (1.0 + dual_step) + spread)
    share = known / groups - (primal_step * scale) * (normal - back_data)
    share = lax.psum_scatter(share.swapaxes(2, 3), "coil", scatter_dimension=2, tiled=True)
    share = share.reshape(width, 2, rows, slabs, planes).transpose(3, 1, 4, 2, 0)
    share = lax.all_to_all(
        share.reshape(slabs, -1), "slab", split_axis=0, concat_axis=0, tiled=True
    ).reshape(slabs, 2, planes, rows, width)
    return share.transpose(1, 2, 3, 0, 4).reshape(2, planes, rows, nx)


def all_planes(ref, coil, turn, part):
    block = ref[:, coil, 0, turn, part]
    return block.reshape(block.shape[0] * block.shape[1], block.shape[2])


def terms(maps, images):
    nz, ny = maps[0][0].shape
    real_sum = imag_sum = None
    for coil, (maps_real, maps_imag) in enumerate(maps):
        real = images[coil * nz : (coil + 1) * nz, :ny]
        imag = images[coil * nz : (coil + 1) * nz, ny:]
        real_term = maps_real * real + maps_imag * imag
        imag_term = maps_real * imag - maps_imag * real
        real_sum = real_term if coil == 0 else real_sum + real_term
        imag_sum = imag_term if coil == 0 else imag_sum + imag_term
    return real_sum, imag_sum


def add_up(out_ref, sums):
    real_sum = functools.reduce(lambda a, b: a + b, [real for real, _ in sums])
    imag_sum = functools.reduce(lambda a, b: a + b, [imag for _, imag in sums])

    @pl.when(pl.program_id(1) == 0)
    def _():
        out_ref[0, 0] = real_sum
        out_ref[0, 1] = imag_sum

    @pl.when(pl.program_id(1) > 0)
    def _():
        out_ref[0, 0] += real_sum
        out_ref[0, 1] += imag_sum


def planes_of(maps_ref, turn):
    return [
        (all_planes(maps_ref, c, turn, 0).astype(f32), all_planes(maps_ref, c, turn, 1).astype(f32))
        for c in range(maps_ref.shape[1])
    ]


def normal_planes(guess_ref, maps_ref, mask_ref, fy_ref, fz_ref, gz_ref, gy_ref, out_ref):
    nz, ny = out_ref.shape[2:]
    group = maps_ref.shape[1]
    guess_real = guess_ref[0, 0]
    guess_imag = guess_ref[0, 1]
    sums = []
    for turn in range(maps_ref.shape[3]):
        maps = planes_of(maps_ref, turn)
        rows = []
        for maps_real, maps_imag in maps:
            real = maps_real * guess_real - maps_imag * guess_imag
            imag = maps_real * guess_imag + maps_imag * guess_real
            rows.append(jnp.concatenate([real.astype(bf16), imag.astype(bf16)], 1))
        pieces = dot(jnp.concatenate(rows, 0), fy_ref[...]).astype(bf16)
        pieces = jnp.concatenate(
            [
                jnp.concatenate(
                    [pieces[c * nz : (c + 1) * nz, j * ny : (j + 1) * ny] for c in range(group)], 1
                )
                for j in range(2)
            ],
            0,
        )
        mask = jnp.concatenate([mask_ref[c, turn] for c in range(group)], 1).astype(f32)
        spectrum = dot(fz_ref[...], pieces) * jnp.concatenate([mask, mask], 0)
        spectrum = spectrum.astype(bf16)
        pieces = dot(gz_ref[...], spectrum).astype(bf16)
        pieces = jnp.concatenate(
            [
                jnp.concatenate(
                    [pieces[j * nz : (j + 1) * nz, c * ny : (c + 1) * ny] for j in range(2)], 1
                )
                for c in range(group)
            ],
            0,
        )
        sums.append(terms(maps, dot(pieces, gy_ref[...])))
    add_up(out_ref, sums)


def back_terms(maps_ref, turn, gz_ref, gy_ref, spectra):
    nz = gz_ref.shape[1] // 2
    shares = spectra[0][0].shape[0]
    spectrum = jnp.concatenate([jnp.concatenate(parts, 1) for parts in spectra], 0)
    pieces = dot(spectrum, gz_ref[...]).astype(bf16)
    columns = jnp.concatenate(
        [
            jnp.concatenate(
                [
                    pieces[c * shares : (c + 1) * shares, j * nz : (j + 1) * nz]
                    for c in range(len(spectra))
                ],
                1,
            )
            for j in range(2)
        ],
        0,
    )
    return terms(planes_of(maps_ref, turn), dot(columns, gy_ref[...], ((0,), (0,))))


def dense_kernel(data_ref, maps_ref, gz_ref, gy_ref, out_ref):
    sums = []
    for turn in range(maps_ref.shape[3]):
        spectra = [
            (all_planes(data_ref, c, turn, 0), all_planes(data_ref, c, turn, 1))
            for c in range(data_ref.shape[1])
        ]
        sums.append(back_terms(maps_ref, turn, gz_ref, gy_ref, spectra))
    add_up(out_ref, sums)


def lanes_at(array, place):
    return jnp.take_along_axis(array, place, 1, mode="promise_in_bounds")


def sparse_kernel(data_ref, code_ref, maps_ref, gz_ref, gy_ref, out_ref):
    half = data_ref.shape[4] // 2
    sums = []
    for turn in range(maps_ref.shape[3]):
        spectra = []
        for coil in range(data_ref.shape[1]):
            lines = data_ref[:, coil, 0, turn].astype(f32)
            lines = [
                lines[:, j * half : (j + 1) * half].reshape(-1, lines.shape[2]) for j in range(2)
            ]
            count = lines[0].shape[0]
            codes = [code_ref[coil, turn, h * count : (h + 1) * count] for h in range(2)]
            spectra.append(
                [
                    jnp.concatenate(
                        [
                            jnp.where(code >= 0, lanes_at(line, jnp.maximum(code, 0)), 0.0)
                            for code in codes
                        ],
                        0,
                    ).astype(bf16)
                    for line in lines
                ]
            )
        sums.append(back_terms(maps_ref, turn, gz_ref, gy_ref, spectra))
    add_up(out_ref, sums)


def select_kernel(edges, pick_ref, data_ref, *out_refs):
    half = data_ref.shape[3] // 2
    lanes = data_ref.shape[4]

    def one(plane_index, _):
        for out_ref, (first, last) in zip(out_refs, edges):
            for coil in range(first, last):
                pick = pick_ref[coil]
                later = pick >= lanes
                place = jnp.where(later, pick - lanes, pick)
                parts = []
                for part in range(2):
                    lines = data_ref[plane_index, coil, part].astype(f32)
                    parts.append(
                        jnp.where(
                            later, lanes_at(lines[half:], place), lanes_at(lines[:half], place)
                        )
                    )
                out_ref[plane_index, coil - first] = jnp.concatenate(parts, 0).astype(bf16)
        return 0

    lax.fori_loop(0, data_ref.shape[0], one, 0)


def selected(data, pick, edges):
    planes, _, _, shares, lanes = data.shape
    step = max(n for n in (1, 2, 4, 8) if planes % n == 0)
    return pl.pallas_call(
        functools.partial(select_kernel, edges),
        out_shape=[
            jax.ShapeDtypeStruct((planes, b - a, shares, lanes), bf16) for a, b in edges
        ],
        grid=(planes // step,),
        in_specs=[
            pl.BlockSpec(pick.shape, lambda x: (0, 0, 0)),
            pl.BlockSpec((step,) + data.shape[1:], lambda x: (x, 0, 0, 0, 0)),
        ],
        out_specs=[
            pl.BlockSpec((step, b - a, shares, lanes), lambda x: (x, 0, 0, 0)) for a, b in edges
        ],
        compiler_params=pltpu.CompilerParams(dimension_semantics=("arbitrary",)),
        cost_estimate=pl.CostEstimate(
            flops=data.size * 64, bytes_accessed=data.size * 3, transcendentals=0
        ),
    )(pick, data)


def deliver_kernel(block_ref, got_ref, send_sem, recv_sem):
    groups = lax.axis_size("coil")
    count = groups * lax.axis_size("slab")
    me = lax.axis_index("slab") * groups + lax.axis_index("coil")
    barrier = pltpu.get_barrier_semaphore()

    def place(step):
        other = lax.rem(me + step, count)
        return other, (lax.rem(other, groups), other // groups)

    def greet(step, _):
        pl.semaphore_signal(
            barrier, inc=1, device_id=place(step)[1], device_id_type=pl.DeviceIdType.MESH
        )
        return 0

    def copy(step):
        other, device = place(step)
        return pltpu.make_async_remote_copy(
            block_ref.at[other],
            got_ref.at[me],
            send_sem.at[step - 1],
            recv_sem.at[step - 1],
            device_id=device,
            device_id_type=pl.DeviceIdType.MESH,
        )

    def begin(step, _):
        copy(step).start()
        return 0

    def end(step, _):
        copy(step).wait()
        return 0

    lax.fori_loop(1, count, greet, 0)
    pl.semaphore_wait(barrier, count - 1)
    lax.fori_loop(1, count, begin, 0)
    got_ref[me] = block_ref[me]
    lax.fori_loop(1, count, end, 0)


def delivered(blocks):
    return pl.pallas_call(
        deliver_kernel,
        out_shape=jax.ShapeDtypeStruct(blocks.shape, blocks.dtype),
        in_specs=[pl.BlockSpec(memory_space=pltpu.VMEM)],
        out_specs=pl.BlockSpec(memory_space=pltpu.VMEM),
        scratch_shapes=[
            pltpu.SemaphoreType.DMA((blocks.shape[0] - 1,)),
            pltpu.SemaphoreType.DMA((blocks.shape[0] - 1,)),
        ],
        compiler_params=pltpu.CompilerParams(collective_id=1, has_side_effects=True),
        cost_estimate=pl.CostEstimate(
            flops=blocks.size * 64, bytes_accessed=blocks.size * 4, transcendentals=0
        ),
    )(blocks)


def share_kernel(own_ref, all_ref, send_sem, recv_sem):
    count = lax.axis_size("slab")
    slab, coil = lax.axis_index("slab"), lax.axis_index("coil")

    def device(step):
        return (coil, lax.rem(slab + step, count))

    barrier = pltpu.get_barrier_semaphore()
    for step in range(1, count):
        pl.semaphore_signal(
            barrier, inc=1, device_id=device(step), device_id_type=pl.DeviceIdType.MESH
        )
    pl.semaphore_wait(barrier, count - 1)
    copies = [
        pltpu.make_async_remote_copy(
            own_ref,
            all_ref.at[slab],
            send_sem.at[step - 1],
            recv_sem.at[step - 1],
            device_id=device(step),
            device_id_type=pl.DeviceIdType.MESH,
        )
        for step in range(1, count)
    ]
    for copy in copies:
        copy.start()
    all_ref[slab] = own_ref[...]
    for copy in copies:
        copy.wait()


def shared(own, slabs):
    return pl.pallas_call(
        share_kernel,
        out_shape=jax.ShapeDtypeStruct((slabs,) + own.shape, own.dtype),
        in_specs=[pl.BlockSpec(memory_space=pltpu.VMEM)],
        out_specs=pl.BlockSpec(memory_space=pltpu.VMEM),
        scratch_shapes=[
            pltpu.SemaphoreType.DMA((slabs - 1,)),
            pltpu.SemaphoreType.DMA((slabs - 1,)),
        ],
        compiler_params=pltpu.CompilerParams(collective_id=0, has_side_effects=True),
        cost_estimate=pl.CostEstimate(
            flops=own.size * 64, bytes_accessed=own.size * 32, transcendentals=0
        ),
    )(own)


def plane_call(kernel, operands, specs, shape, steps, flops, nbytes):
    return pl.pallas_call(
        kernel,
        out_shape=jax.ShapeDtypeStruct(shape, f32),
        grid=(shape[0], steps),
        in_specs=specs,
        out_specs=pl.BlockSpec((1,) + shape[1:], lambda x, c: (x, 0, 0, 0)),
        compiler_params=pltpu.CompilerParams(
            dimension_semantics=("arbitrary", "arbitrary"), vmem_limit_bytes=48 * 2**20
        ),
        cost_estimate=pl.CostEstimate(flops=flops, bytes_accessed=nbytes, transcendentals=0),
    )(*operands)


def every_source(array, turns, start=0):
    slabs, groups, _, _, *rest = array.shape
    return pl.BlockSpec(
        (slabs, groups, 1, turns, *rest),
        lambda x, c: (0, 0, x, start + c) + (0,) * len(rest),
    )


def per_coil(array, turns, start=0):
    return pl.BlockSpec(
        (array.shape[0], turns) + array.shape[2:], lambda x, c: (0, start + c, 0, 0)
    )


def normal_of(guess, maps, mask, tables):
    shape = guess.shape
    groups, coils = maps.shape[1], maps.shape[3]
    turns = math.gcd(coils, 4)
    specs = [
        pl.BlockSpec((1,) + shape[1:], lambda x, c: (x, 0, 0, 0)),
        every_source(maps, turns),
        per_coil(mask, turns),
    ] + [whole(t.shape) for t in tables]
    cells = groups * coils * shape[0] * shape[2] * shape[3]
    operands = (guess, maps, mask) + tables
    steps = coils // turns
    return plane_call(normal_planes, operands, specs, shape, steps, cells * 4096, cells * 4)


def back_of(data, code, maps, tables, shape, start):
    groups, coils = maps.shape[1], data.shape[3]
    turns = math.gcd(math.gcd(coils, start), 2)
    steps, start = coils // turns, start // turns
    operands, specs = [data], [every_source(data, turns)]
    if code is not None:
        operands.append(code)
        specs.append(per_coil(code, turns, start))
    operands += (maps,) + tables
    specs += [every_source(maps, turns, start)] + [whole(t.shape) for t in tables]
    cells = groups * coils * shape[0] * shape[2] * shape[3]
    kernel = dense_kernel if code is None else sparse_kernel
    return plane_call(kernel, operands, specs, shape, steps, cells * 2048, cells * 8)


EVERY = ("slab", "coil")
LANES = 128
SUBLANES = 8


def ranks(flags):
    size = flags.shape[-1]
    flags = flags.astype(bf16)

    def count(table):
        sums = jnp.einsum("...k,kl->...l", flags, table, preferred_element_type=f32)
        return sums.astype(jnp.int32)

    every = jnp.ones((size, size), bf16)
    return count(jnp.triu(every)), count(every)


def swap(blocks):
    return lax.all_to_all(blocks, EVERY, split_axis=0, concat_axis=0, tiled=True)


def tv_planes(guess, duals, first, total):
    here, ahead = guess[:-1], guess[1:]
    pos = first - 1 + lax.broadcasted_iota(jnp.int32, (here.shape[0], 1, 1, 1), 0)
    grad_x = jnp.where(pos < total - 1, ahead - here, 0.0)
    grad_z = jnp.concatenate([here[:, :, 1:] - here[:, :, :-1], jnp.zeros_like(here[:, :, :1])], 2)
    grad_y = jnp.concatenate([here[..., 1:] - here[..., :-1], jnp.zeros_like(here[..., :1])], 3)
    moved = [dual_step * grad for grad in (grad_z, grad_y, grad_x)]
    if duals is not None:
        moved = [dual + step for dual, step in zip(duals, moved)]
    magnitude = jnp.sqrt(sum(jnp.sum(w * w, 1, keepdims=True) for w in moved))
    factor = 1.0 / jnp.maximum(1.0, magnitude / tv_weight)
    duals = [w * factor for w in moved]
    dual_z, dual_y = duals[0][1:], duals[1][1:]
    dual_x = jnp.where(pos < 0, 0.0, duals[2])
    spread_x = dual_x[:-1] - dual_x[1:]
    spread_z = jnp.concatenate([jnp.zeros_like(dual_z[:, :, :1]), dual_z[:, :, :-1]], 2) - dual_z
    spread_y = jnp.concatenate([jnp.zeros_like(dual_y[..., :1]), dual_y[..., :-1]], 3) - dual_y
    return duals, spread_z + spread_y + spread_x


def by_planes(kspace_data, coil_maps, sample_mask, initial_image):
    slabs = lax.axis_size("slab")
    groups = lax.axis_size("coil")
    devices = slabs * groups
    coils, _, depth, ny, nx = coil_maps.shape
    nz, shares = kspace_data.shape[2:4]
    rows = initial_image.shape[2]
    width = nx // devices
    me = lax.axis_index(EVERY)
    forward_y, inverse_y = dft_table(ny, False), dft_table(ny, True)
    forward_z, inverse_z = dft_table(nz, False), dft_table(nz, True)
    inverse_x = jnp.asarray(dft_table(nx, True))
    tables = (on_right(forward_y), on_left(forward_z), on_left(inverse_z), on_right(inverse_y))
    hold = lax.optimization_barrier

    def packed(array):
        return array.reshape((devices, width) + array.shape[1:])

    def sent(array):
        return swap(array).reshape((slabs, groups) + array.shape[1:])

    def in_place(array):
        order = Layout(major_to_minor=tuple(range(array.ndim)))
        return with_layout_constraint(array, order)

    image = initial_image.reshape(-1, nx).astype(bf16).T.reshape(devices, width, -1)
    edge = jnp.zeros_like(image[:1, :1])
    image = jnp.concatenate(
        [
            jnp.concatenate([edge, image[:-1, -1:]], 0),
            image,
            jnp.concatenate([image[1:, :1], edge], 0),
        ],
        1,
    )
    image = image.reshape(devices, -1, ny)
    image, coil_maps = hold((image, coil_maps))
    image = swap(image)
    mask = shared(sample_mask.swapaxes(1, 2).astype(bf16), slabs)
    maps = packed(coil_maps.transpose(4, 0, 1, 2, 3))
    image, mask, maps = hold((image, mask, maps))
    maps = sent(maps)

    image = image.reshape(slabs, groups, width + 2, 2, depth, rows)
    image = image.transpose(2, 3, 0, 4, 1, 5).reshape(width + 2, 2, nz, ny)
    image = hold(image).astype(f32)
    own = image[1:-1]

    data = kspace_data * sample_mask[:, None, :, :, None].astype(bf16)
    data = jnp.einsum("ckzyx,kjxw->wcjyz", data, inverse_x, preferred_element_type=f32)
    data = in_place(data.astype(bf16))
    half = shares // 2
    small = half == SUBLANES and nz == LANES
    last = max(1, coils // 4)
    edges = [(0, coils - last), (coils - last, coils)]
    if small:
        sampled = sample_mask.swapaxes(1, 2)
        rank, total = ranks(sampled)
        begin = total[:, :half]
        kz = lax.broadcasted_iota(jnp.int32, (1, 1, nz), 2)
        slot = jnp.where(sampled > 0, rank, 0)
        second = jnp.where(sampled[:, half:] > 0, begin + slot[:, half:], 0)
        slot = jnp.concatenate([slot[:, :half], second], 2)
        spot = jnp.arange(2 * nz, dtype=jnp.int32)
        pick = jnp.sum(
            jnp.where(slot[:, :, None, :] == 1 + kz[..., None], spot, 0), 3, dtype=jnp.int32
        )
        lines = [packed(piece) for piece in selected(data, pick, edges)]
        data, lines, mask = hold((data, lines, mask))
    else:
        data, mask = hold((data, mask))
    mask = mask.swapaxes(0, 1).reshape(coils, slabs * shares, nz)
    masks = []
    for part in (mask[: coils // 2], mask[coils // 2 :]):
        if masks:
            part, _ = hold((part, masks[0]))
        masks.append(lax.all_gather(part, "coil", axis=0))
    mask = jnp.concatenate(masks, 1)

    inverse = (on_right(inverse_z), on_right(inverse_y))
    if small:
        halves = hold(mask.reshape(groups, coils, slabs, 2, half, nz).swapaxes(2, 3))
        rank, total = ranks(halves)
        begin = total[:, :, :1]
        fits = jnp.max(begin + total[:, :, 1:]) <= nz
        rank = jnp.concatenate([rank[:, :, :1], begin + rank[:, :, 1:]], 2)
        code = jnp.where(halves > 0, rank - 1, -1).reshape(groups, coils, ny, nz)
        order = np.arange(ny).reshape(slabs, 2, half).swapaxes(0, 1).reshape(-1)
        sparse_inverse = (inverse[0], inverse[1].reshape(2, ny, -1)[:, order].reshape(2 * ny, -1))
    mask = mask.swapaxes(2, 3)
    duals, spread = tv_planes(image, None, me * width, nx)
    held = (maps, mask, data, own, duals, spread)
    if small:
        (maps, mask, data, own, duals, spread), lines, code = hold((held, lines, code))
    else:
        maps, mask, data, own, duals, spread = hold(held)

    def finish(pieces, code, inverse):
        normal = normal_of(own, maps, mask, tables)
        back, start = None, 0
        for turn in range(len(pieces)):
            got = sent(pieces[turn])
            if turn == 0:
                got, normal, pieces = hold((got, normal, pieces))
            term = back_of(got, code, maps, inverse, own.shape, start)
            back = term if back is None else back + term
            start += got.shape[3]
        return normal, back

    def dense(_):
        return finish([packed(data)], None, inverse)

    def sparse(_):
        return finish(lines, code, sparse_inverse)

    normal, back = lax.cond(fits, sparse, dense, 0) if small else dense(0)
    scale = dual_step / (1.0 + dual_step)
    data_grad = scale * (normal - back)
    change = -primal_step * (data_grad + spread)
    guess = own + 2.0 * change
    line = [g * slabs + s for s in range(slabs) for g in range(groups)]
    before = lax.ppermute(guess[-1:], ("coil", "slab"), list(zip(line[:-1], line[1:])))
    after = lax.ppermute(guess[:1], ("coil", "slab"), list(zip(line[1:], line[:-1])))
    normal = normal_of(guess, maps, mask, tables)
    _, spread = tv_planes(jnp.concatenate([before, guess, after], 0), duals, me * width, nx)
    data_grad = data_grad / (1.0 + dual_step) + scale * (normal - back)
    final = (own + change - primal_step * (data_grad + spread)).astype(bf16)
    final = final.reshape(width, 2, slabs, depth, groups, rows).transpose(2, 4, 0, 1, 3, 5)
    final = delivered(final.reshape(devices, -1, LANES)).reshape(nx, -1).T
    return final.reshape(initial_image.shape).astype(f32)


def solution(mesh):
    placed = (
        P("coil", None, None, "slab", None),
        P("coil", None, "slab", None, None),
        P("coil", None, "slab"),
        P(None, "slab", "coil", None),
    )

    def on_each(kspace_data, coil_maps, sample_mask, initial_image):
        whole_planes = coil_maps.shape[4] % mesh.size == 0
        form = by_planes if whole_planes else on_device
        return form(kspace_data, coil_maps, sample_mask, initial_image)

    return jax.shard_map(
        on_each,
        mesh=mesh,
        in_specs=placed,
        out_specs=P(None, "slab", "coil", None),
        check_vma=False,
    )
```

```python
import functools
import math

import jax
import jax.numpy as jnp
import ml_dtypes
import numpy as np
from jax import lax
from jax.experimental import pallas as pl
from jax.experimental.layout import Layout, with_layout_constraint
from jax.experimental.pallas import tpu as pltpu
from jax.sharding import PartitionSpec as P


dual_step = 0.25
primal_step = 0.25
tv_weight = 0.5
f32 = jnp.float32
bf16 = jnp.bfloat16


def from_behind(block, axis, distance):
    devices = range(lax.axis_size(axis))
    route = [(i - distance, i) for i in devices if i - distance in devices]
    return lax.ppermute(block, axis, route)


def dft_table(length, inverse):
    counter = np.arange(length)
    phase = 2.0 * math.pi / length * (np.outer(counter, counter) % length)
    real_part = np.cos(phase) / math.sqrt(length)
    imag_part = np.sin(phase) / math.sqrt(length)
    if not inverse:
        imag_part = -imag_part
    table = np.stack([np.stack([real_part, imag_part]), np.stack([-imag_part, real_part])])
    return table.astype(ml_dtypes.bfloat16)


def on_right(table):
    n = table.shape[2]
    return jnp.asarray(table.transpose(0, 2, 1, 3).reshape(2 * n, 2 * n))


def on_left(table):
    n = table.shape[2]
    return jnp.asarray(table.transpose(1, 3, 0, 2).reshape(2 * n, 2 * n))


def plane(ref, coil, part):
    block = ref[:, coil, 0, part]
    return block.reshape(block.shape[0] * block.shape[1], block.shape[2])


def dot(a, b, dims=((1,), (0,))):
    return lax.dot_general(a, b, (dims, ((), ())), preferred_element_type=f32)


def combine(out_ref, maps_ref, images, group):
    nz, ny = out_ref.shape[2:]
    real_sum = imag_sum = None
    for coil in range(group):
        real = images[coil * nz : (coil + 1) * nz, :ny]
        imag = images[coil * nz : (coil + 1) * nz, ny:]
        maps_real = plane(maps_ref, coil, 0).astype(f32)
        maps_imag = plane(maps_ref, coil, 1).astype(f32)
        real_term = maps_real * real + maps_imag * imag
        imag_term = maps_real * imag - maps_imag * real
        real_sum = real_term if coil == 0 else real_sum + real_term
        imag_sum = imag_term if coil == 0 else imag_sum + imag_term

    @pl.when(pl.program_id(1) == 0)
    def _():
        out_ref[0, 0] = real_sum
        out_ref[0, 1] = imag_sum

    @pl.when(pl.program_id(1) > 0)
    def _():
        out_ref[0, 0] += real_sum
        out_ref[0, 1] += imag_sum


def normal_kernel(group, guess_ref, maps_ref, mask_ref, fy_ref, fz_ref, gz_ref, gy_ref, out_ref):
    nz, ny = out_ref.shape[2:]
    guess_real = guess_ref[0, 0]
    guess_imag = guess_ref[0, 1]
    rows = []
    for coil in range(group):
        maps_real = plane(maps_ref, coil, 0).astype(f32)
        maps_imag = plane(maps_ref, coil, 1).astype(f32)
        real = maps_real * guess_real - maps_imag * guess_imag
        imag = maps_real * guess_imag + maps_imag * guess_real
        rows.append(jnp.concatenate([real.astype(bf16), imag.astype(bf16)], 1))
    pieces = dot(jnp.concatenate(rows, 0), fy_ref[...]).astype(bf16)
    pieces = jnp.concatenate(
        [
            jnp.concatenate(
                [pieces[c * nz : (c + 1) * nz, j * ny : (j + 1) * ny] for c in range(group)], 1
            )
            for j in range(2)
        ],
        0,
    )
    spectrum = dot(fz_ref[...], pieces).astype(bf16)
    mask = jnp.concatenate([mask_ref[c] for c in range(group)], 1)
    spectrum = spectrum * jnp.concatenate([mask, mask], 0)
    pieces = dot(gz_ref[...], spectrum).astype(bf16)
    pieces = jnp.concatenate(
        [
            jnp.concatenate(
                [pieces[j * nz : (j + 1) * nz, c * ny : (c + 1) * ny] for j in range(2)], 1
            )
            for c in range(group)
        ],
        0,
    )
    combine(out_ref, maps_ref, dot(pieces, gy_ref[...]), group)


def data_kernel(group, data_ref, maps_ref, gy_ref, out_ref):
    columns = jnp.concatenate(
        [
            jnp.concatenate([plane(data_ref, c, 0), plane(data_ref, c, 1)], 0)
            for c in range(group)
        ],
        1,
    )
    combine(out_ref, maps_ref, dot(columns, gy_ref[...], ((0,), (0,))), group)


def whole(shape):
    return pl.BlockSpec(shape, lambda x, c: (0,) * len(shape))


def coil_blocks(array, group):
    src, _, _, parts, planes, cols = array.shape
    return pl.BlockSpec((src, group, 1, parts, planes, cols), lambda x, c: (0, c, x, 0, 0, 0))


def call(kernel, group, operands, specs, shape, coils, flops, nbytes):
    return pl.pallas_call(
        functools.partial(kernel, group),
        out_shape=jax.ShapeDtypeStruct(shape, f32),
        grid=(shape[0], coils // group),
        in_specs=specs,
        out_specs=pl.BlockSpec((1,) + shape[1:], lambda x, c: (x, 0, 0, 0)),
        compiler_params=pltpu.CompilerParams(
            dimension_semantics=("arbitrary", "arbitrary"), vmem_limit_bytes=48 * 2**20
        ),
        cost_estimate=pl.CostEstimate(flops=flops, bytes_accessed=nbytes, transcendentals=0),
    )(*operands)


def coil_group(coils):
    return max(g for g in (1, 2, 4) if coils % g == 0)


def apply_normal(guess, maps, mask, tables):
    coils = maps.shape[1]
    group = coil_group(coils)
    shape = guess.shape
    specs = [
        pl.BlockSpec((1,) + shape[1:], lambda x, c: (x, 0, 0, 0)),
        coil_blocks(maps, group),
        pl.BlockSpec((group,) + mask.shape[1:], lambda x, c: (c, 0, 0)),
    ] + [whole(t.shape) for t in tables]
    cells = coils * shape[0] * shape[2] * shape[3]
    return call(
        normal_kernel, group, (guess, maps, mask) + tables, specs, shape, coils, cells * 4096, cells * 4
    )


def apply_data(data, maps, table, shape):
    coils = maps.shape[1]
    group = coil_group(coils)
    specs = [coil_blocks(data, group), coil_blocks(maps, group), whole(table.shape)]
    cells = coils * shape[0] * shape[2] * shape[3]
    return call(data_kernel, group, (data, maps, table), specs, shape, coils, cells * 1024, cells * 8)


def exchange(blocks):
    got = lax.all_to_all(blocks, "slab", split_axis=0, concat_axis=0, tiled=True)
    if got.shape[4] % 16:
        src, coils, width, parts, share, cols = got.shape
        got = got.transpose(1, 2, 3, 0, 4, 5).reshape(1, coils, width, parts, src * share, cols)
    return got


def tv_update(guess, duals):
    width = guess.shape[0]
    size = lax.axis_size("slab") * width
    pos = lax.axis_index("slab") * width + lax.broadcasted_iota(jnp.int32, (width, 1, 1, 1), 0)
    ahead_x = jnp.concatenate([guess[1:], from_behind(guess[:1], "slab", -1)], 0)
    grad_x = jnp.where(pos < size - 1, ahead_x - guess, 0.0)
    grad_z = jnp.concatenate(
        [guess[:, :, 1:] - guess[:, :, :-1], jnp.zeros_like(guess[:, :, :1])], 2
    )
    grad_y = jnp.concatenate([guess[..., 1:] - guess[..., :-1], jnp.zeros_like(guess[..., :1])], 3)
    moved = [dual_step * grad for grad in (grad_z, grad_y, grad_x)]
    if duals is not None:
        moved = [dual + step for dual, step in zip(duals, moved)]
    magnitude = jnp.sqrt(sum(jnp.sum(w * w, 1, keepdims=True) for w in moved))
    factor = 1.0 / jnp.maximum(1.0, magnitude / tv_weight)
    dual_z, dual_y, dual_x = [w * factor for w in moved]
    prior = from_behind(dual_x[-1:], "slab", 1)
    spread_x = jnp.concatenate([prior, dual_x[:-1]], 0) - dual_x
    spread_z = jnp.concatenate([jnp.zeros_like(dual_z[:, :, :1]), dual_z[:, :, :-1]], 2) - dual_z
    spread_y = jnp.concatenate([jnp.zeros_like(dual_y[..., :1]), dual_y[..., :-1]], 3) - dual_y
    return (dual_z, dual_y, dual_x), spread_z + spread_y + spread_x


def on_device(kspace_data, coil_maps, sample_mask, initial_image):
    slabs = lax.axis_size("slab")
    groups = lax.axis_size("coil")
    coils, _, planes, ny, nx = coil_maps.shape
    nz = kspace_data.shape[2]
    shares = kspace_data.shape[3]
    rows = initial_image.shape[2]
    width = nx // slabs
    forward_y, inverse_y = dft_table(ny, False), dft_table(ny, True)
    forward_z, inverse_z = dft_table(nz, False), dft_table(nz, True)
    inverse_x = jnp.asarray(dft_table(nx, True))
    tables = (on_right(forward_y), on_left(forward_z), on_left(inverse_z), on_right(inverse_y))

    image = initial_image.reshape(2, planes, rows, slabs, width).transpose(3, 4, 0, 2, 1)
    image = lax.all_to_all(
        image.reshape(slabs, -1), "slab", split_axis=0, concat_axis=0, tiled=True
    ).reshape(slabs, width, 2, rows, planes)
    image = image.transpose(1, 2, 3, 0, 4).reshape(width, 2, rows, nz)
    image = lax.all_gather(image, "coil", axis=2, tiled=True).swapaxes(2, 3)
    mask = lax.all_gather(sample_mask.astype(bf16), "slab", axis=2, tiled=True)

    maps = coil_maps.reshape(coils, 2, planes, ny, slabs, width).transpose(4, 0, 5, 1, 2, 3)
    maps, image, mask = lax.optimization_barrier((maps, image, mask))
    maps = exchange(maps)

    data = kspace_data * sample_mask[:, None, :, :, None].astype(bf16)
    data = jnp.einsum("ckzyx,kjxw->cjzyw", data, inverse_x, preferred_element_type=f32).astype(bf16)
    data = jnp.einsum(
        "ckzyx,kjzw->cjywx", data, jnp.asarray(inverse_z), preferred_element_type=f32
    ).astype(bf16)
    data = data.reshape(coils, 2, shares, nz, slabs, width).transpose(4, 0, 5, 1, 2, 3)
    data, maps = lax.optimization_barrier((data, maps))
    data = exchange(data)

    normal = apply_normal(image, maps, mask, tables)
    duals, spread = tv_update(image, None)
    data, normal, duals, spread = lax.optimization_barrier((data, normal, duals, spread))
    back_data = apply_data(data, maps, tables[3], image.shape)
    scale = dual_step / (1.0 + dual_step)
    data_grad = lax.psum(scale * (normal - back_data), "coil")
    updated = image - primal_step * (data_grad + spread)
    guess = 2.0 * updated - image
    normal = apply_normal(guess, maps, mask, tables)
    _, spread = tv_update(guess, duals)
    known = updated - primal_step * (data_grad / (1.0 + dual_step) + spread)
    share = known / groups - (primal_step * scale) * (normal - back_data)
    share = lax.psum_scatter(share.swapaxes(2, 3), "coil", scatter_dimension=2, tiled=True)
    share = share.reshape(width, 2, rows, slabs, planes).transpose(3, 1, 4, 2, 0)
    share = lax.all_to_all(
        share.reshape(slabs, -1), "slab", split_axis=0, concat_axis=0, tiled=True
    ).reshape(slabs, 2, planes, rows, width)
    return share.transpose(1, 2, 3, 0, 4).reshape(2, planes, rows, nx)


def all_planes(ref, coil, turn, part):
    block = ref[:, coil, 0, turn, part]
    return block.reshape(block.shape[0] * block.shape[1], block.shape[2])


def terms(maps, images):
    nz, ny = maps[0][0].shape
    real_sum = imag_sum = None
    for coil, (maps_real, maps_imag) in enumerate(maps):
        real = images[coil * nz : (coil + 1) * nz, :ny]
        imag = images[coil * nz : (coil + 1) * nz, ny:]
        real_term = maps_real * real + maps_imag * imag
        imag_term = maps_real * imag - maps_imag * real
        real_sum = real_term if coil == 0 else real_sum + real_term
        imag_sum = imag_term if coil == 0 else imag_sum + imag_term
    return real_sum, imag_sum


def add_up(out_ref, sums):
    real_sum = functools.reduce(lambda a, b: a + b, [real for real, _ in sums])
    imag_sum = functools.reduce(lambda a, b: a + b, [imag for _, imag in sums])

    @pl.when(pl.program_id(1) == 0)
    def _():
        out_ref[0, 0] = real_sum
        out_ref[0, 1] = imag_sum

    @pl.when(pl.program_id(1) > 0)
    def _():
        out_ref[0, 0] += real_sum
        out_ref[0, 1] += imag_sum


def planes_of(maps_ref, turn):
    return [
        (all_planes(maps_ref, c, turn, 0).astype(f32), all_planes(maps_ref, c, turn, 1).astype(f32))
        for c in range(maps_ref.shape[1])
    ]


def normal_planes(guess_ref, maps_ref, mask_ref, fy_ref, fz_ref, gz_ref, gy_ref, out_ref):
    nz, ny = out_ref.shape[2:]
    group = maps_ref.shape[1]
    guess_real = guess_ref[0, 0]
    guess_imag = guess_ref[0, 1]
    sums = []
    for turn in range(maps_ref.shape[3]):
        maps = planes_of(maps_ref, turn)
        rows = []
        for maps_real, maps_imag in maps:
            real = maps_real * guess_real - maps_imag * guess_imag
            imag = maps_real * guess_imag + maps_imag * guess_real
            rows.append(jnp.concatenate([real.astype(bf16), imag.astype(bf16)], 1))
        pieces = dot(jnp.concatenate(rows, 0), fy_ref[...]).astype(bf16)
        pieces = jnp.concatenate(
            [
                jnp.concatenate(
                    [pieces[c * nz : (c + 1) * nz, j * ny : (j + 1) * ny] for c in range(group)], 1
                )
                for j in range(2)
            ],
            0,
        )
        mask = jnp.concatenate([mask_ref[c, turn] for c in range(group)], 1).astype(f32)
        spectrum = dot(fz_ref[...], pieces) * jnp.concatenate([mask, mask], 0)
        spectrum = spectrum.astype(bf16)
        pieces = dot(gz_ref[...], spectrum).astype(bf16)
        pieces = jnp.concatenate(
            [
                jnp.concatenate(
                    [pieces[j * nz : (j + 1) * nz, c * ny : (c + 1) * ny] for j in range(2)], 1
                )
                for c in range(group)
            ],
            0,
        )
        sums.append(terms(maps, dot(pieces, gy_ref[...])))
    add_up(out_ref, sums)


def back_terms(maps_ref, turn, gz_ref, gy_ref, spectra):
    nz = gz_ref.shape[1] // 2
    shares = spectra[0][0].shape[0]
    spectrum = jnp.concatenate([jnp.concatenate(parts, 1) for parts in spectra], 0)
    pieces = dot(spectrum, gz_ref[...]).astype(bf16)
    columns = jnp.concatenate(
        [
            jnp.concatenate(
                [
                    pieces[c * shares : (c + 1) * shares, j * nz : (j + 1) * nz]
                    for c in range(len(spectra))
                ],
                1,
            )
            for j in range(2)
        ],
        0,
    )
    return terms(planes_of(maps_ref, turn), dot(columns, gy_ref[...], ((0,), (0,))))


def dense_kernel(data_ref, maps_ref, gz_ref, gy_ref, out_ref):
    sums = []
    for turn in range(maps_ref.shape[3]):
        spectra = [
            (all_planes(data_ref, c, turn, 0), all_planes(data_ref, c, turn, 1))
            for c in range(data_ref.shape[1])
        ]
        sums.append(back_terms(maps_ref, turn, gz_ref, gy_ref, spectra))
    add_up(out_ref, sums)


def lanes_at(array, place):
    return jnp.take_along_axis(array, place, 1, mode="promise_in_bounds")


def sparse_kernel(data_ref, code_ref, maps_ref, gz_ref, gy_ref, out_ref):
    half = data_ref.shape[4] // 2
    sums = []
    for turn in range(maps_ref.shape[3]):
        spectra = []
        for coil in range(data_ref.shape[1]):
            lines = data_ref[:, coil, 0, turn].astype(f32)
            lines = [
                lines[:, j * half : (j + 1) * half].reshape(-1, lines.shape[2]) for j in range(2)
            ]
            count = lines[0].shape[0]
            codes = [code_ref[coil, turn, h * count : (h + 1) * count] for h in range(2)]
            spectra.append(
                [
                    jnp.concatenate(
                        [
                            jnp.where(code >= 0, lanes_at(line, jnp.maximum(code, 0)), 0.0)
                            for code in codes
                        ],
                        0,
                    ).astype(bf16)
                    for line in lines
                ]
            )
        sums.append(back_terms(maps_ref, turn, gz_ref, gy_ref, spectra))
    add_up(out_ref, sums)


def select_kernel(edges, pick_ref, data_ref, *out_refs):
    half = data_ref.shape[3] // 2
    lanes = data_ref.shape[4]

    def one(plane_index, _):
        for out_ref, (first, last) in zip(out_refs, edges):
            for coil in range(first, last):
                pick = pick_ref[coil]
                later = pick >= lanes
                place = jnp.where(later, pick - lanes, pick)
                parts = []
                for part in range(2):
                    lines = data_ref[plane_index, coil, part].astype(f32)
                    parts.append(
                        jnp.where(
                            later, lanes_at(lines[half:], place), lanes_at(lines[:half], place)
                        )
                    )
                out_ref[plane_index, coil - first] = jnp.concatenate(parts, 0).astype(bf16)
        return 0

    lax.fori_loop(0, data_ref.shape[0], one, 0)


def selected(data, pick, edges):
    planes, _, _, shares, lanes = data.shape
    step = max(n for n in (1, 2, 4, 8) if planes % n == 0)
    return pl.pallas_call(
        functools.partial(select_kernel, edges),
        out_shape=[
            jax.ShapeDtypeStruct((planes, b - a, shares, lanes), bf16) for a, b in edges
        ],
        grid=(planes // step,),
        in_specs=[
            pl.BlockSpec(pick.shape, lambda x: (0, 0, 0)),
            pl.BlockSpec((step,) + data.shape[1:], lambda x: (x, 0, 0, 0, 0)),
        ],
        out_specs=[
            pl.BlockSpec((step, b - a, shares, lanes), lambda x: (x, 0, 0, 0)) for a, b in edges
        ],
        compiler_params=pltpu.CompilerParams(dimension_semantics=("arbitrary",)),
        cost_estimate=pl.CostEstimate(
            flops=data.size * 64, bytes_accessed=data.size * 3, transcendentals=0
        ),
    )(pick, data)


def deliver_kernel(block_ref, got_ref, send_sem, recv_sem):
    groups = lax.axis_size("coil")
    count = groups * lax.axis_size("slab")
    me = lax.axis_index("slab") * groups + lax.axis_index("coil")
    barrier = pltpu.get_barrier_semaphore()

    def place(step):
        other = lax.rem(me + step, count)
        return other, (lax.rem(other, groups), other // groups)

    def greet(step, _):
        pl.semaphore_signal(
            barrier, inc=1, device_id=place(step)[1], device_id_type=pl.DeviceIdType.MESH
        )
        return 0

    def copy(step):
        other, device = place(step)
        return pltpu.make_async_remote_copy(
            block_ref.at[other],
            got_ref.at[me],
            send_sem.at[step - 1],
            recv_sem.at[step - 1],
            device_id=device,
            device_id_type=pl.DeviceIdType.MESH,
        )

    def begin(step, _):
        copy(1 + lax.rem(step - 1 + count // 2 - 1, count - 1)).start()
        return 0

    def end(step, _):
        copy(step).wait()
        return 0

    lax.fori_loop(1, count, greet, 0)
    pl.semaphore_wait(barrier, count - 1)
    lax.fori_loop(1, count, begin, 0)
    got_ref[me] = block_ref[me]
    lax.fori_loop(1, count, end, 0)


def delivered(blocks):
    return pl.pallas_call(
        deliver_kernel,
        out_shape=jax.ShapeDtypeStruct(blocks.shape, blocks.dtype),
        in_specs=[pl.BlockSpec(memory_space=pltpu.VMEM)],
        out_specs=pl.BlockSpec(memory_space=pltpu.VMEM),
        scratch_shapes=[
            pltpu.SemaphoreType.DMA((blocks.shape[0] - 1,)),
            pltpu.SemaphoreType.DMA((blocks.shape[0] - 1,)),
        ],
        compiler_params=pltpu.CompilerParams(collective_id=1, has_side_effects=True),
        cost_estimate=pl.CostEstimate(
            flops=blocks.size * 64, bytes_accessed=blocks.size * 4, transcendentals=0
        ),
    )(blocks)


def share_kernel(own_ref, all_ref, send_sem, recv_sem):
    count = lax.axis_size("slab")
    slab, coil = lax.axis_index("slab"), lax.axis_index("coil")

    def device(step):
        return (coil, lax.rem(slab + step, count))

    barrier = pltpu.get_barrier_semaphore()
    for step in range(1, count):
        pl.semaphore_signal(
            barrier, inc=1, device_id=device(step), device_id_type=pl.DeviceIdType.MESH
        )
    pl.semaphore_wait(barrier, count - 1)
    copies = [
        pltpu.make_async_remote_copy(
            own_ref,
            all_ref.at[slab],
            send_sem.at[step - 1],
            recv_sem.at[step - 1],
            device_id=device(step),
            device_id_type=pl.DeviceIdType.MESH,
        )
        for step in range(1, count)
    ]
    far = count // 2 - 1
    for copy in copies[far:] + copies[:far]:
        copy.start()
    all_ref[slab] = own_ref[...]
    for copy in copies:
        copy.wait()


def shared(own, slabs):
    return pl.pallas_call(
        share_kernel,
        out_shape=jax.ShapeDtypeStruct((slabs,) + own.shape, own.dtype),
        in_specs=[pl.BlockSpec(memory_space=pltpu.VMEM)],
        out_specs=pl.BlockSpec(memory_space=pltpu.VMEM),
        scratch_shapes=[
            pltpu.SemaphoreType.DMA((slabs - 1,)),
            pltpu.SemaphoreType.DMA((slabs - 1,)),
        ],
        compiler_params=pltpu.CompilerParams(collective_id=0, has_side_effects=True),
        cost_estimate=pl.CostEstimate(
            flops=own.size * 64, bytes_accessed=own.size * 32, transcendentals=0
        ),
    )(own)


def plane_call(kernel, operands, specs, shape, steps, flops, nbytes):
    return pl.pallas_call(
        kernel,
        out_shape=jax.ShapeDtypeStruct(shape, f32),
        grid=(shape[0], steps),
        in_specs=specs,
        out_specs=pl.BlockSpec((1,) + shape[1:], lambda x, c: (x, 0, 0, 0)),
        compiler_params=pltpu.CompilerParams(
            dimension_semantics=("arbitrary", "arbitrary"), vmem_limit_bytes=48 * 2**20
        ),
        cost_estimate=pl.CostEstimate(flops=flops, bytes_accessed=nbytes, transcendentals=0),
    )(*operands)


def every_source(array, turns, start=0):
    slabs, groups, _, _, *rest = array.shape
    return pl.BlockSpec(
        (slabs, groups, 1, turns, *rest),
        lambda x, c: (0, 0, x, start + c) + (0,) * len(rest),
    )


def per_coil(array, turns, start=0):
    return pl.BlockSpec(
        (array.shape[0], turns) + array.shape[2:], lambda x, c: (0, start + c, 0, 0)
    )


def normal_of(guess, maps, mask, tables):
    shape = guess.shape
    groups, coils = maps.shape[1], maps.shape[3]
    turns = math.gcd(coils, 4)
    specs = [
        pl.BlockSpec((1,) + shape[1:], lambda x, c: (x, 0, 0, 0)),
        every_source(maps, turns),
        per_coil(mask, turns),
    ] + [whole(t.shape) for t in tables]
    cells = groups * coils * shape[0] * shape[2] * shape[3]
    operands = (guess, maps, mask) + tables
    steps = coils // turns
    return plane_call(normal_planes, operands, specs, shape, steps, cells * 4096, cells * 4)


def back_of(data, code, maps, tables, shape, start):
    groups, coils = maps.shape[1], data.shape[3]
    turns = math.gcd(math.gcd(coils, start), 2)
    steps, start = coils // turns, start // turns
    operands, specs = [data], [every_source(data, turns)]
    if code is not None:
        operands.append(code)
        specs.append(per_coil(code, turns, start))
    operands += (maps,) + tables
    specs += [every_source(maps, turns, start)] + [whole(t.shape) for t in tables]
    cells = groups * coils * shape[0] * shape[2] * shape[3]
    kernel = dense_kernel if code is None else sparse_kernel
    return plane_call(kernel, operands, specs, shape, steps, cells * 2048, cells * 8)


EVERY = ("slab", "coil")
LANES = 128
SUBLANES = 8


def ranks(flags):
    size = flags.shape[-1]
    flags = flags.astype(bf16)

    def count(table):
        sums = jnp.einsum("...k,kl->...l", flags, table, preferred_element_type=f32)
        return sums.astype(jnp.int32)

    every = jnp.ones((size, size), bf16)
    return count(jnp.triu(every)), count(every)


def swap(blocks):
    return lax.all_to_all(blocks, EVERY, split_axis=0, concat_axis=0, tiled=True)


def tv_planes(guess, duals, first, total):
    here, ahead = guess[:-1], guess[1:]
    pos = first - 1 + lax.broadcasted_iota(jnp.int32, (here.shape[0], 1, 1, 1), 0)
    grad_x = jnp.where(pos < total - 1, ahead - here, 0.0)
    grad_z = jnp.concatenate([here[:, :, 1:] - here[:, :, :-1], jnp.zeros_like(here[:, :, :1])], 2)
    grad_y = jnp.concatenate([here[..., 1:] - here[..., :-1], jnp.zeros_like(here[..., :1])], 3)
    moved = [dual_step * grad for grad in (grad_z, grad_y, grad_x)]
    if duals is not None:
        moved = [dual + step for dual, step in zip(duals, moved)]
    magnitude = jnp.sqrt(sum(jnp.sum(w * w, 1, keepdims=True) for w in moved))
    factor = 1.0 / jnp.maximum(1.0, magnitude / tv_weight)
    duals = [w * factor for w in moved]
    dual_z, dual_y = duals[0][1:], duals[1][1:]
    dual_x = jnp.where(pos < 0, 0.0, duals[2])
    spread_x = dual_x[:-1] - dual_x[1:]
    spread_z = jnp.concatenate([jnp.zeros_like(dual_z[:, :, :1]), dual_z[:, :, :-1]], 2) - dual_z
    spread_y = jnp.concatenate([jnp.zeros_like(dual_y[..., :1]), dual_y[..., :-1]], 3) - dual_y
    return duals, spread_z + spread_y + spread_x


def by_planes(kspace_data, coil_maps, sample_mask, initial_image):
    slabs = lax.axis_size("slab")
    groups = lax.axis_size("coil")
    devices = slabs * groups
    coils, _, depth, ny, nx = coil_maps.shape
    nz, shares = kspace_data.shape[2:4]
    rows = initial_image.shape[2]
    width = nx // devices
    me = lax.axis_index(EVERY)
    forward_y, inverse_y = dft_table(ny, False), dft_table(ny, True)
    forward_z, inverse_z = dft_table(nz, False), dft_table(nz, True)
    inverse_x = jnp.asarray(dft_table(nx, True))
    tables = (on_right(forward_y), on_left(forward_z), on_left(inverse_z), on_right(inverse_y))
    hold = lax.optimization_barrier

    def packed(array):
        return array.reshape((devices, width) + array.shape[1:])

    def sent(array):
        return swap(array).reshape((slabs, groups) + array.shape[1:])

    def in_place(array):
        order = Layout(major_to_minor=tuple(range(array.ndim)))
        return with_layout_constraint(array, order)

    image = initial_image.reshape(-1, nx).astype(bf16).T.reshape(devices, width, -1)
    edge = jnp.zeros_like(image[:1, :1])
    image = jnp.concatenate(
        [
            jnp.concatenate([edge, image[:-1, -1:]], 0),
            image,
            jnp.concatenate([image[1:, :1], edge], 0),
        ],
        1,
    )
    image = image.reshape(devices, -1, ny)
    image, coil_maps = hold((image, coil_maps))
    image = swap(image)
    mask = shared(sample_mask.swapaxes(1, 2).astype(bf16), slabs)
    maps = packed(coil_maps.transpose(4, 0, 1, 2, 3))
    image, mask, maps = hold((image, mask, maps))
    maps = sent(maps)

    image = image.reshape(slabs, groups, width + 2, 2, depth, rows)
    image = image.transpose(2, 3, 0, 4, 1, 5).reshape(width + 2, 2, nz, ny)
    image = hold(image).astype(f32)
    own = image[1:-1]

    data = kspace_data * sample_mask[:, None, :, :, None].astype(bf16)
    data = jnp.einsum("ckzyx,kjxw->wcjyz", data, inverse_x, preferred_element_type=f32)
    data = in_place(data.astype(bf16))
    half = shares // 2
    small = half == SUBLANES and nz == LANES
    last = max(1, coils // 4)
    edges = [(0, coils - last), (coils - last, coils)]
    if small:
        sampled = sample_mask.swapaxes(1, 2)
        rank, total = ranks(sampled)
        begin = total[:, :half]
        kz = lax.broadcasted_iota(jnp.int32, (1, 1, nz), 2)
        slot = jnp.where(sampled > 0, rank, 0)
        second = jnp.where(sampled[:, half:] > 0, begin + slot[:, half:], 0)
        slot = jnp.concatenate([slot[:, :half], second], 2)
        spot = jnp.arange(2 * nz, dtype=jnp.int32)
        pick = jnp.sum(
            jnp.where(slot[:, :, None, :] == 1 + kz[..., None], spot, 0), 3, dtype=jnp.int32
        )
        lines = [packed(piece) for piece in selected(data, pick, edges)]
        data, lines, mask = hold((data, lines, mask))
    else:
        data, mask = hold((data, mask))
    mask = mask.swapaxes(0, 1).reshape(coils, slabs * shares, nz)
    masks = []
    for part in (mask[: coils // 2], mask[coils // 2 :]):
        if masks:
            part, _ = hold((part, masks[0]))
        masks.append(lax.all_gather(part, "coil", axis=0))
    mask = jnp.concatenate(masks, 1)

    inverse = (on_right(inverse_z), on_right(inverse_y))
    if small:
        halves = hold(mask.reshape(groups, coils, slabs, 2, half, nz).swapaxes(2, 3))
        rank, total = ranks(halves)
        begin = total[:, :, :1]
        fits = jnp.max(begin + total[:, :, 1:]) <= nz
        rank = jnp.concatenate([rank[:, :, :1], begin + rank[:, :, 1:]], 2)
        code = jnp.where(halves > 0, rank - 1, -1).reshape(groups, coils, ny, nz)
        order = np.arange(ny).reshape(slabs, 2, half).swapaxes(0, 1).reshape(-1)
        sparse_inverse = (inverse[0], inverse[1].reshape(2, ny, -1)[:, order].reshape(2 * ny, -1))
    mask = mask.swapaxes(2, 3)
    duals, spread = tv_planes(image, None, me * width, nx)
    held = (maps, mask, data, own, duals, spread)
    if small:
        (maps, mask, data, own, duals, spread), lines, code = hold((held, lines, code))
    else:
        maps, mask, data, own, duals, spread = hold(held)

    def finish(pieces, code, inverse):
        normal = normal_of(own, maps, mask, tables)
        back, start = None, 0
        for turn in range(len(pieces)):
            got = sent(pieces[turn])
            if turn == 0:
                got, normal, pieces = hold((got, normal, pieces))
            term = back_of(got, code, maps, inverse, own.shape, start)
            back = term if back is None else back + term
            start += got.shape[3]
        return normal, back

    def dense(_):
        return finish([packed(data)], None, inverse)

    def sparse(_):
        return finish(lines, code, sparse_inverse)

    normal, back = lax.cond(fits, sparse, dense, 0) if small else dense(0)
    scale = dual_step / (1.0 + dual_step)
    data_grad = scale * (normal - back)
    change = -primal_step * (data_grad + spread)
    guess = own + 2.0 * change
    line = [g * slabs + s for s in range(slabs) for g in range(groups)]
    before = lax.ppermute(guess[-1:], ("coil", "slab"), list(zip(line[:-1], line[1:])))
    after = lax.ppermute(guess[:1], ("coil", "slab"), list(zip(line[1:], line[:-1])))
    normal = normal_of(guess, maps, mask, tables)
    _, spread = tv_planes(jnp.concatenate([before, guess, after], 0), duals, me * width, nx)
    data_grad = data_grad / (1.0 + dual_step) + scale * (normal - back)
    final = (own + change - primal_step * (data_grad + spread)).astype(bf16)
    final = final.reshape(width, 2, slabs, depth, groups, rows).transpose(2, 4, 0, 1, 3, 5)
    final = delivered(final.reshape(devices, -1, LANES)).reshape(nx, -1).T
    return final.reshape(initial_image.shape).astype(f32)


def solution(mesh):
    placed = (
        P("coil", None, None, "slab", None),
        P("coil", None, "slab", None, None),
        P("coil", None, "slab"),
        P(None, "slab", "coil", None),
    )

    def on_each(kspace_data, coil_maps, sample_mask, initial_image):
        whole_planes = coil_maps.shape[4] % mesh.size == 0
        form = by_planes if whole_planes else on_device
        return form(kspace_data, coil_maps, sample_mask, initial_image)

    return jax.shard_map(
        on_each,
        mesh=mesh,
        in_specs=placed,
        out_specs=P(None, "slab", "coil", None),
        check_vma=False,
    )
```
